32 devices in a mesh: dp: 4 (over z), row: 4 (over x, core), col: 2 (over y).
Axes of the slice: x: 2, y: 2, z: 4, core: 2. Of those that a mesh axis runs over, the one named last changes fastest.
Arguments:
- tokens: float32 [768, 8192], P('row', ('dp', 'col')), may hold values from -6 to 6
- cotangent: float32 [768, 8192], P('row', ('dp', 'col')), may hold values from -6 to 6
- offsets: int32 [8, 2], P(('dp', 'col')), may hold values from 0 to 10
- ln1_gain: float32 [768], replicated, may hold values from 0.5 to 1.5
- ln1_bias: float32 [768], replicated, may hold values from -4 to 4
- q_weight: float32 [768, 768], P('row', 'col'), may hold values from -0.21875 to 0.21875
- k_weight: float32 [768, 768], P('row', 'col'), may hold values from -0.21875 to 0.21875
- v_weight: float32 [768, 768], P('row', 'col'), may hold values from -0.21875 to 0.21875
- q_bias: float32 [768], replicated, may hold values from -4 to 4
- v_bias: float32 [768], replicated, may hold values from -4 to 4
- rel_pos_h: float32 [27, 64], replicated, may hold values from -1.5 to 1.5
- rel_pos_w: float32 [27, 64], replicated, may hold values from -1.5 to 1.5
- out_weight: float32 [768, 768], P('row', 'col'), may hold values from -1.5 to 1.5
- out_bias: float32 [768], replicated, may hold values from -4 to 4
- ln2_gain: float32 [768], replicated, may hold values from 0.5 to 1.5
- ln2_bias: float32 [768], replicated, may hold values from -4 to 4
- up_weight: float32 [768, 3072], P('row', 'col'), may hold values from -0.21875 to 0.21875
- up_bias: float32 [3072], replicated, may hold values from -6 to 6
- down_weight: float32 [3072, 768], P('row', 'col'), may hold values from -0.109375 to 0.109375
- down_bias: float32 [768], replicated, may hold values from -4 to 4
Outputs:
- output: float32 [768, 8192], P('row', ('dp', 'col'))
- input_grad: float32 [768, 8192], P('row', ('dp', 'col'))
- ln1_gain_grad: float32 [768], replicated
- ln1_bias_grad: float32 [768], replicated
- q_weight_grad: float32 [768, 768], P('row', 'col')
- k_weight_grad: float32 [768, 768], P('row', 'col')
- v_weight_grad: float32 [768, 768], P('row', 'col')
- q_bias_grad: float32 [768], replicated
- v_bias_grad: float32 [768], replicated
- rel_pos_h_grad: float32 [27, 64], replicated
- rel_pos_w_grad: float32 [27, 64], replicated
- out_weight_grad: float32 [768, 768], P('row', 'col')
- out_bias_grad: float32 [768], replicated
- ln2_gain_grad: float32 [768], replicated
- ln2_bias_grad: float32 [768], replicated
- up_weight_grad: float32 [768, 3072], P('row', 'col')
- up_bias_grad: float32 [3072], replicated
- down_weight_grad: float32 [3072, 768], P('row', 'col')
- down_bias_grad: float32 [768], replicated
The draws below stay inside these ranges and needn't reach their ends.
Inputs may be any that keep to these rules, and one draw needn't show every extreme that they name: `offsets`: row and column of each image's first token inside its padded grid of 42 x 42 cells.
All inputs are finite; a program needn't handle non-finite values.
Results may differ from the reference program's by a relative error of at most 0.012.
The reference program's roundings to bfloat16 on the way count: a program that leaves them out, or rounds other values in their place, can miss the bound.
Values may be sent and summed in bfloat16 or wider, within the bound.
A program may use at most 128 MiB of HBM per device.

```python
import jax
import jax.numpy as jnp
from jax import lax

D = 768
HEADS = 12
HEAD_DIM = 64
MLP = 3072
WIN = 14
SIDE = 32
PSIDE = 42
IMAGES = 8
TOKENS = 8192


def plant(array, stream_key, smallest, top_value):
    longest = array.shape.index(max(array.shape))
    spots = []
    for shift in (0, 1):
        where = [jax.random.randint(jax.random.fold_in(stream_key, axis), (), 0, length) for axis, length in enumerate(array.shape)]
        where[longest] = (where[longest] + shift) % array.shape[longest]
        spots.append(tuple(where))
    return array.at[spots[0]].set(smallest).at[spots[1]].set(top_value)


def shard_levels(key, extent, cuts, smallest, top_value):
    factor_of = 1.0
    for position, parts in cuts:
        heights = jax.random.uniform(jax.random.fold_in(jax.random.fold_in(key, 6), position), (parts,), jnp.float32, smallest / len(cuts), top_value / len(cuts))
        factor_of = factor_of * jnp.repeat(jnp.exp(heights), extent[position] // parts).reshape((-1,) + (1,) * (len(extent) - 1 - position))
    return factor_of


def gaussian(key, dims, deviation, reach, shards=(), held_as=jnp.bfloat16):
    values = jax.random.normal(key, dims, jnp.float32) * deviation
    if len(shards) > 0:
        values = shard_levels(key, dims, shards, -0.22, 0.18) * values
    return jnp.clip(values, min=-reach, max=reach).astype(held_as)


def setup_inputs(seed: int = 0) -> dict:
    seeds = jax.random.split(jax.random.key(seed), 21)
    return {
        "tokens": gaussian(seeds[0], (D, TOKENS), 1.0, 6.0, ((0, 4), (1, 8)), jnp.float32),
        "cotangent": gaussian(seeds[1], (D, TOKENS), 1.0, 6.0, ((0, 4), (1, 8)), jnp.float32),
        "offsets": plant(jax.random.randint(seeds[2], (IMAGES, 2), 0, PSIDE - SIDE + 1), jax.random.fold_in(seeds[2], 1), 0, PSIDE - SIDE).astype(jnp.int32),
        "ln1_gain": jnp.clip(1.0 + 0.1 * jax.random.normal(seeds[3], (D,), jnp.float32), 0.5, 1.5),
        "ln1_bias": gaussian(seeds[4], (D,), 0.3, 4.0, (), jnp.float32),
        "q_weight": gaussian(seeds[5], (D, D), D ** -0.5, 0.21875, ((0, 4), (1, 2)), jnp.float32),
        "k_weight": gaussian(seeds[6], (D, D), D ** -0.5, 0.21875, ((0, 4), (1, 2)), jnp.float32),
        "v_weight": gaussian(seeds[7], (D, D), D ** -0.5, 0.21875, ((0, 4), (1, 2)), jnp.float32),
        "q_bias": gaussian(seeds[8], (D,), 0.3, 4.0, (), jnp.float32),
        "v_bias": gaussian(seeds[9], (D,), 0.3, 4.0, (), jnp.float32),
        "rel_pos_h": gaussian(seeds[10], (2 * WIN - 1, HEAD_DIM), 0.1, 1.5, (), jnp.float32),
        "rel_pos_w": gaussian(seeds[11], (2 * WIN - 1, HEAD_DIM), 0.1, 1.5, (), jnp.float32),
        "out_weight": gaussian(seeds[12], (D, D), (max(D // 48, 1)) ** -0.5, 1.5, ((0, 4), (1, 2)), jnp.float32),
        "out_bias": gaussian(seeds[13], (D,), 0.3, 4.0, (), jnp.float32),
        "ln2_gain": jnp.clip(1.0 + 0.1 * jax.random.normal(seeds[14], (D,), jnp.float32), 0.5, 1.5),
        "ln2_bias": gaussian(seeds[15], (D,), 0.3, 4.0, (), jnp.float32),
        "up_weight": gaussian(seeds[16], (D, MLP), D ** -0.5, 0.21875, ((0, 4), (1, 2)), jnp.float32),
        "up_bias": gaussian(seeds[17], (MLP,), 0.5, 6.0, (), jnp.float32),
        "down_weight": gaussian(seeds[18], (MLP, D), MLP ** -0.5, 0.109375, ((0, 4), (1, 2)), jnp.float32),
        "down_bias": gaussian(seeds[19], (D,), 0.3, 4.0, (), jnp.float32),
    }


epsilon = 1e-06
MASKED = -1e+30
HIGHEST = lax.Precision.HIGHEST

@jax.custom_vjp
def low(v):
    return lax.optimization_barrier(v.astype(jnp.bfloat16)).astype(jnp.float32)

@jax.custom_vjp
def low_back(v):
    return v

def low_keep(v):
    return (low(v), None)

def low_pass(kept, grad):
    return (grad,)

def back_keep(v):
    return (v, None)

def back_low(kept, grad):
    return (low(grad),)
low.defvjp(low_keep, low_pass)
low_back.defvjp(back_keep, back_low)

def matmul(first_op, second_op):
    return jnp.dot(first_op, second_op, precision=HIGHEST, preferred_element_type=jnp.float32)

def layer_norm(source, gain, shift):
    average = lax.optimization_barrier(jnp.mean(source, axis=-1, keepdims=True))
    spread = lax.optimization_barrier(jnp.mean(source * source, axis=-1, keepdims=True)) - average * average
    return (source - average) * lax.rsqrt(spread + epsilon) * gain + shift

def to_windows(source, offset):
    channels = source.shape[-1]
    blocks_side = PSIDE // WIN
    image_grid = source.reshape(SIDE, SIDE, channels)
    padded = jnp.zeros((PSIDE, PSIDE, channels), source.dtype)
    padded = lax.dynamic_update_slice(padded, image_grid, (offset[0], offset[1], jnp.int32(0)))
    blocks = padded.reshape(blocks_side, WIN, blocks_side, WIN, channels).transpose(0, 2, 1, 3, 4)
    return blocks.reshape(blocks_side * blocks_side, WIN * WIN, channels)

def from_windows(blocks, offset):
    channels = blocks.shape[-1]
    blocks_side = PSIDE // WIN
    padded = blocks.reshape(blocks_side, blocks_side, WIN, WIN, channels).transpose(0, 2, 1, 3, 4)
    padded = padded.reshape(PSIDE, PSIDE, channels)
    image_grid = lax.dynamic_slice(padded, (offset[0], offset[1], jnp.int32(0)), (SIDE, SIDE, channels))
    return image_grid.reshape(SIDE * SIDE, channels)

def key_valid(offset):
    blocks_side = PSIDE // WIN
    coords = jnp.arange(PSIDE, dtype=jnp.int32)
    in_rows = (coords >= offset[0]) & (coords < offset[0] + SIDE)
    in_cols = (coords >= offset[1]) & (coords < offset[1] + SIDE)
    usable = (in_rows[:, None] & in_cols[None, :]).astype(jnp.int32)
    usable = usable.reshape(blocks_side, WIN, blocks_side, WIN).transpose(0, 2, 1, 3)
    return usable.reshape(blocks_side * blocks_side, WIN * WIN)

def rel_table(rel_pos):
    coords = jnp.arange(WIN, dtype=jnp.int32)
    rel_index = coords[:, None] - coords[None, :] + WIN - 1
    one_hot = (rel_index[:, :, None] == jnp.arange(2 * WIN - 1, dtype=jnp.int32)[None, None, :]).astype(jnp.float32)
    return jnp.einsum('ijr,rc->ijc', one_hot, rel_pos, precision=HIGHEST)

def attention(queries, key_rows, value_rows, offset, table_rows, table_cols):
    window_count = (PSIDE // WIN) ** 2
    query_win = to_windows(queries, offset).reshape(window_count, WIN * WIN, HEADS, HEAD_DIM)
    key_win = to_windows(key_rows, offset).reshape(window_count, WIN * WIN, HEADS, HEAD_DIM)
    value_win = to_windows(value_rows, offset).reshape(window_count, WIN * WIN, HEADS, HEAD_DIM)
    direct = jnp.einsum('nqhc,nkhc->nhqk', query_win * HEAD_DIM ** (-0.5), key_win, precision=HIGHEST)
    query_grid = query_win.reshape(window_count, WIN, WIN, HEADS, HEAD_DIM)
    along_rows = jnp.einsum('nyxhc,ykc->nhyxk', query_grid, table_rows, precision=HIGHEST)
    along_cols = jnp.einsum('nyxhc,xkc->nhyxk', query_grid, table_cols, precision=HIGHEST)
    scores = direct.reshape(window_count, HEADS, WIN, WIN, WIN, WIN) + along_rows[..., :, None] + along_cols[..., None, :]
    scores = low_back(scores.reshape(window_count, HEADS, WIN * WIN, WIN * WIN))
    usable = key_valid(offset)
    scores = jnp.where(usable[:, None, None, :] > 0, scores, MASKED)
    weights = low(jax.nn.softmax(scores, axis=-1))
    mixed = jnp.einsum('nhqk,nkhc->nqhc', weights, value_win, precision=HIGHEST)
    return from_windows(mixed.reshape(window_count, WIN * WIN, D), offset)

def block(inputs, offset, params):
    first_gain, first_shift, w_query, w_key, w_value, b_query, b_value, rel_rows, rel_cols, w_out, b_out, second_gain, second_shift, w_up, b_up, w_down, b_down = params
    first_in = low(layer_norm(inputs, first_gain, first_shift))
    queries = low(low_back(matmul(first_in, low(w_query)) + b_query))
    key_rows = low(low_back(matmul(first_in, low(w_key))))
    value_rows = low(low_back(matmul(first_in, low(w_value)) + b_value))
    table_rows = rel_table(low(rel_rows))
    table_cols = rel_table(low(rel_cols))
    attended = low(low_back(attention(queries, key_rows, value_rows, offset, table_rows, table_cols)))
    middle = inputs + low_back(matmul(attended, low(w_out)) + b_out)
    second_in = low(layer_norm(middle, second_gain, second_shift))
    hidden_pre = low_back(matmul(second_in, low(w_up)) + b_up)
    hidden_act = low(jax.nn.gelu(hidden_pre, approximate=False))
    return middle + low_back(matmul(hidden_act, low(w_down)) + b_down)

def reference(tokens, cotangent, offsets, ln1_gain, ln1_bias, q_weight, k_weight, v_weight, q_bias, v_bias, rel_pos_h, rel_pos_w, out_weight, out_bias, ln2_gain, ln2_bias, up_weight, up_bias, down_weight, down_bias):
    params = (ln1_gain, ln1_bias, q_weight, k_weight, v_weight, q_bias, v_bias, rel_pos_h, rel_pos_w, out_weight, out_bias, ln2_gain, ln2_bias, up_weight, up_bias, down_weight, down_bias)

    def one_image(running, pieces):
        image, upstream, offset = pieces

        def forward(inputs, weights):
            return block(inputs, offset, weights)
        result, pullback = jax.vjp(forward, image, params)
        input_grad, param_grads = pullback(upstream)
        return (jax.tree.map(jnp.add, running, param_grads), (result, input_grad))
    initial = jax.tree.map(jnp.zeros_like, params)
    images = tokens.T.reshape(IMAGES, SIDE * SIDE, D)
    upstreams = cotangent.T.reshape(IMAGES, SIDE * SIDE, D)
    summed, (outputs, input_grads) = lax.scan(one_image, initial, (images, upstreams, offsets))
    return (outputs.reshape(TOKENS, D).T, input_grads.reshape(TOKENS, D).T) + tuple(summed)
```

```python
import functools
import jax, jax.numpy as jnp
from jax import lax
from jax.sharding import PartitionSpec as P
from jax.experimental import pallas as pl
from jax.experimental.pallas import tpu as pltpu

WIN=14; SIDE=32; CELL=16; GRIDW=48; PAD=10; NEG=-1e30
SLOTS=((0,128),(128,128),(256,128),(384,64),(448,64),(512,64))
f32=jnp.float32; bf16=jnp.bfloat16

def nt(a,b): return lax.dot_general(a,b,(((1,),(1,)),((),())),preferred_element_type=f32)
def nn(a,b): return lax.dot_general(a,b,(((1,),(0,)),((),())),preferred_element_type=f32)
def tn(a,b): return lax.dot_general(a,b,(((0,),(0,)),((),())),preferred_element_type=f32)

def codes():
    i=jnp.arange(8*GRIDW,dtype=jnp.int32); cell=i%GRIDW; xx=cell%CELL
    cells=jnp.where(xx<WIN,(i//GRIDW)*1000+(cell//CELL)*WIN+xx,-100000)
    j=jnp.arange(8*SIDE,dtype=jnp.int32)
    toks=(j//SIDE)*1000+j%SIDE
    return cells,toks

def rel_operands(rel_h,rel_w):
    h=rel_h[::-1].astype(bf16).T; w=rel_w[::-1].astype(bf16).T
    z=jnp.zeros((2,128,256),bf16)
    n=2*WIN-1
    z=z.at[0,0:64,64:64+n].set(h).at[0,0:64,128+65:128+65+n].set(w)
    z=z.at[1,64:128,0:n].set(h).at[1,64:128,128+1:128+1+n].set(w)
    return z

def spot_to_cells(slot_ref,src,cells_col,toks_row,c0):
    pass

def place(z,feat,spots,dmat,g):
    for row,width,lane in spots:
        got=nt(dmat,feat[row:row+width,256*g:256*(g+1)]).astype(bf16)
        z[pl.ds(PAD+8*g,8),:,lane:lane+width]=got.reshape(8,GRIDW,width)

def head_consts():
    lane=lax.broadcasted_iota(jnp.int32,(WIN,CELL,128),2)
    y=lax.broadcasted_iota(jnp.int32,(WIN,CELL,128),0)
    x=lax.broadcasted_iota(jnp.int32,(WIN,CELL,128),1)
    return lane,y,x

def skew(t,sign):
    th=t[:,0:128]; tw=t[:,128:256]
    outs=[]; outw=[]
    for y in range(WIN):
        a=th[CELL*y:CELL*(y+1)]
        s=(sign*(y-13))%128
        outs.append(pltpu.roll(a,s,1) if s else a)
        if sign>0:
            outw.append(pltpu.roll(tw[CELL*y:CELL*(y+1)],0,1,stride=1,stride_axis=0))
    if sign<0:
        x=lax.broadcasted_iota(jnp.int32,(WIN*CELL,128),0)&(CELL-1)
        for bit in (1,2,4,8):
            tw=jnp.where((x&bit)>0,pltpu.roll(tw,128-bit,1),tw)
        outw=[tw]
    return jnp.concatenate(outs,0),jnp.concatenate(outw,0)

def query_operand(q,rel,base,lane2,own):
    t=nn(q,rel)
    a,b=skew(t,1)
    in_h=(lane2>=base)&(lane2<base+WIN); in_w=(lane2>=base+WIN)&(lane2<base+2*WIN)
    both=jnp.where(in_h,a,jnp.where(in_w,b,0.0))
    hi=both.astype(bf16)
    lo=(both-hi.astype(f32)).astype(bf16)
    one=(lane2==base+2*WIN).astype(f32)
    first=(q.astype(f32)*0.125+hi.astype(f32)+one).astype(bf16)
    return jnp.concatenate([first,lo],1)

def key_operand(k,base,wy,wx,r0,c0):
    lane,y,x=head_consts()
    g=WIN*wy+y-r0; c=WIN*wx+x-c0
    ok=(g>=0)&(g<SIDE)&(c>=0)&(c<SIDE)&(x<WIN)
    eye=(((lane-base)==y)|((lane-base-WIN)==x)&(x<WIN)).astype(f32)
    eye=eye.reshape(WIN*CELL,128)
    mask=jnp.where((lane==base+2*WIN)&jnp.logical_not(ok),NEG,0.0).reshape(WIN*CELL,128)
    first=(k.astype(f32)+eye+mask).astype(bf16)
    return jnp.concatenate([first,eye.astype(bf16)],1)

HEADS3=((0,128*0,0),(1,128*0,0),(0,128*3,1))

def load_win(z,wy,wx,r0,lane):
    row=WIN*wy-r0+PAD
    return z[pl.ds(row,WIN),pl.ds(pl.multiple_of(CELL*wx,CELL),CELL),lane:lane+128].reshape(WIN*CELL,128)

def half_mask(v,half,lane2):
    keep=(lane2<64) if half==0 else (lane2>=64)
    return jnp.where(keep,v.astype(f32),0.0).astype(bf16)

def fwd_kernel(off,qkv,rel,cells,toks,o_ref,z,ow):
    r0=off[0,0]; c0=off[0,1]
    dmat=((cells[...]-c0)==toks[...]).astype(f32).astype(bf16)
    z[0:PAD]=jnp.zeros((PAD,GRIDW,768),bf16)
    z[PAD+SIDE:]=jnp.zeros((PAD,GRIDW,768),bf16)
    for lane in (384,512,640):
        z[PAD:PAD+SIDE,:,lane:lane+128]=jnp.zeros((SIDE,GRIDW,128),bf16)
    spots=[(r,w,128*i) for i,(r,w) in enumerate(SLOTS)]
    for g in range(4): place(z,qkv,spots,dmat,g)
    def window(n,carry):
        wy=n//3; wx=n%3
        lane2=lax.broadcasted_iota(jnp.int32,(WIN*CELL,128),1)
        for pair in range(2):
            q=load_win(z,wy,wx,r0,384*pair); k=load_win(z,wy,wx,r0,384*pair+128); v=load_win(z,wy,wx,r0,384*pair+256)
            total=None
            for half in range(2-pair):
                base=64 if half==0 else 0
                qq=half_mask(q,half,lane2); kk=half_mask(k,half,lane2)
                qc=query_operand(qq,rel[half],base,lane2,half)
                kc=key_operand(kk,base,wy,wx,r0,c0)
                s=nt(qc,kc)
                m=jnp.max(s,axis=1,keepdims=True)
                e=jnp.exp(s-m)
                p=(e*(1.0/jnp.sum(e,axis=1,keepdims=True))).astype(bf16)
                o=nn(p,v)
                total=o if total is None else jnp.where(lane2<64,total,o)
            ow[pl.ds(WIN*wy,WIN),pl.ds(pl.multiple_of(CELL*wx,CELL),CELL),128*pair:128*pair+128]=total.astype(bf16).reshape(WIN,CELL,128)
        return carry
    lax.fori_loop(0,9,window,0)
    for g in range(4):
        rows=ow[pl.ds(r0+8*g,8)].reshape(8*GRIDW,256)
        got=tn(dmat,rows)
        o_ref[256*g:256*(g+1),0:192]=got[:,0:192].astype(bf16)

def attend(off,qkv,rel):
    cells,toks=codes()
    return pl.pallas_call(fwd_kernel,out_shape=jax.ShapeDtypeStruct((1024,192),bf16),
      in_specs=[pl.BlockSpec(memory_space=pltpu.SMEM)]+[pl.BlockSpec(memory_space=pltpu.VMEM)]*4,
      out_specs=pl.BlockSpec(memory_space=pltpu.VMEM),
      scratch_shapes=[pltpu.VMEM((SIDE+2*PAD,GRIDW,768),bf16),pltpu.VMEM((42,GRIDW,256),bf16)],
      compiler_params=pltpu.CompilerParams(vmem_limit_bytes=56<<20),name="attend",
    )(off,qkv,rel,cells[:,None],toks[None,:])

def bwd_kernel(off,qkv,do,rel,cells,toks,g_ref,drel_ref,z,gw,tw):
    r0=off[0,0]; c0=off[0,1]
    dmat=((cells[...]-c0)==toks[...]).astype(f32).astype(bf16)
    z[0:PAD]=jnp.zeros((PAD,GRIDW,1024),bf16)
    z[PAD+SIDE:]=jnp.zeros((PAD,GRIDW,1024),bf16)
    for lane in (384,512,640,896):
        z[PAD:PAD+SIDE,:,lane:lane+128]=jnp.zeros((SIDE,GRIDW,128),bf16)
    spots=[(r,w,128*i) for i,(r,w) in enumerate(SLOTS)]
    for g in range(4):
        place(z,qkv,spots,dmat,g)
        place(z,do,((0,128,768),(128,64,896)),dmat,g)
    drel_ref[...]=jnp.zeros(drel_ref.shape,f32)
    def window(n,carry):
        wy=n//3; wx=n%3
        lane2=lax.broadcasted_iota(jnp.int32,(WIN*CELL,128),1)
        lane4=lax.broadcasted_iota(jnp.int32,(WIN*CELL,256),1)
        for pair in range(2):
            q=load_win(z,wy,wx,r0,384*pair); k=load_win(z,wy,wx,r0,384*pair+128); v=load_win(z,wy,wx,r0,384*pair+256)
            d=load_win(z,wy,wx,r0,768+128*pair)
            dq=dk=dv=None
            for half in range(2-pair):
                base=64 if half==0 else 0
                qq=half_mask(q,half,lane2); kk=half_mask(k,half,lane2); dd=half_mask(d,half,lane2)
                qc=query_operand(qq,rel[half],base,lane2,half)
                kc=key_operand(kk,base,wy,wx,r0,c0)
                s=nt(qc,kc)
                m=jnp.max(s,axis=1,keepdims=True)
                e=jnp.exp(s-m)
                p=e*(1.0/jnp.sum(e,axis=1,keepdims=True))
                pb=p.astype(bf16)
                dp=nt(dd,v)
                centre=jnp.sum(p*dp,axis=1,keepdims=True)
                ds=(p*(dp-centre)).astype(bf16)
                dvh=tn(pb,dd)
                dkh=tn(ds,qq)*0.125
                dqc=nn(ds,kc[:,0:128])
                t=jnp.concatenate([jnp.where((lane2>=base)&(lane2<base+WIN),dqc,0.0),
                                   jnp.where((lane2>=base+WIN)&(lane2<base+2*WIN),dqc,0.0)],1)
                a,b=skew(t,-1)
                t=jnp.concatenate([a,b],1)
                thi=t.astype(bf16)
                tlo=(t-thi.astype(f32)).astype(bf16)
                own=(lane2<64) if half==0 else (lane2>=64)
                dqh=jnp.where(own,dqc*0.125,0.0)+nt(thi,rel[half])+nt(tlo,rel[half])
                drel_ref[half]+=tn(qq,thi)
                if dq is None: dq,dk,dv=dqh,dkh,dvh
                else: dq,dk,dv=dq+dqh,dk+dkh,dv+dvh
            rows=pl.ds(WIN*wy,WIN); cols=pl.ds(pl.multiple_of(CELL*wx,CELL),CELL)
            for i,val in enumerate((dq,dk,dv)):
                lane=384*pair+128*i
                gw[rows,cols,lane:lane+128]=val.astype(bf16).reshape(WIN,CELL,128)
        return carry
    lax.fori_loop(0,9,window,0)
    for g in range(4):
        for i,(r,w) in enumerate(SLOTS):
            rows=gw[pl.ds(r0+8*g,8),:,128*i:128*i+128].reshape(8*GRIDW,128)
            got=tn(dmat,rows)
            g_ref[256*g:256*(g+1),r:r+w]=got[:,0:w].astype(bf16)

def attend_back(off,qkv,do,rel):
    cells,toks=codes()
    return pl.pallas_call(bwd_kernel,out_shape=(jax.ShapeDtypeStruct((1024,576),bf16),jax.ShapeDtypeStruct((2,128,256),f32)),
      in_specs=[pl.BlockSpec(memory_space=pltpu.SMEM)]+[pl.BlockSpec(memory_space=pltpu.VMEM)]*5,
      out_specs=(pl.BlockSpec(memory_space=pltpu.VMEM),)*2,
      scratch_shapes=[pltpu.VMEM((SIDE+2*PAD,GRIDW,1024),bf16),pltpu.VMEM((42,GRIDW,768),bf16),pltpu.VMEM((8,128),f32)],
      compiler_params=pltpu.CompilerParams(vmem_limit_bytes=56<<20),name="attend_back",
    )(off,qkv,do,rel,cells[:,None],toks[None,:])

def rel_grads(drel):
    n=2*WIN-1
    h=drel[0,0:64,64:64+n]+drel[1,64:128,0:n]
    w=drel[0,0:64,193:193+n]+drel[1,64:128,129:129+n]
    return h.T[::-1],w.T[::-1]

EPS=1e-06
D=768

def gelu_parts(h):
    cdf=0.5*(1.0+lax.erf(h*0.7071067811865476))
    pdf=jnp.exp(-0.5*h*h)*0.3989422804014327
    return h*cdf,cdf+h*pdf

def own_rows(vector,length,place):
    return lax.dynamic_slice_in_dim(vector,place*length,length,0)

def spread(portion,whole,place):
    return lax.dynamic_update_slice_in_dim(jnp.zeros((whole,),f32),portion,place*portion.shape[0],0)

def head_order(q,k,v):
    return jnp.concatenate([q[...,0:128],k[...,0:128],v[...,0:128],q[...,128:],k[...,128:],v[...,128:]],-1)

def head_unorder(m):
    cat=lambda a,b:jnp.concatenate([m[...,a:a+128],m[...,b:b+64]],-1)
    return cat(0,384),cat(128,448),cat(256,512)

def gather_rows(block):
    return lax.all_gather(block,"row",axis=0,tiled=True)

def sum_rows(partial):
    return lax.psum_scatter(partial.astype(bf16),"row",scatter_dimension=0,tiled=True).astype(f32)

def row_stats(*vals):
    both=lax.psum(jnp.stack([jnp.sum(v,axis=0) for v in vals]),"row")
    return [both[i:i+1]/D for i in range(len(vals))]

def local(tokens,cotangent,offsets,ln1_gain,ln1_bias,q_weight,k_weight,v_weight,q_bias,v_bias,rel_pos_h,rel_pos_w,
          out_weight,out_bias,ln2_gain,ln2_bias,up_weight,up_bias,down_weight,down_bias):
    rows=lax.axis_size("row"); r=lax.axis_index("row"); cols=lax.axis_size("col")
    width=tokens.shape[0]; hidden=up_bias.shape[0]//rows
    gather_col=lambda w:lax.all_gather(w.astype(bf16),"col",axis=1,tiled=True)
    per=rows//cols
    def quarters(w):
        n=w.shape[1]//per
        return [w[:,n*i:n*i+n].astype(bf16) for i in range(per)]
    qs=[head_order(a,b,c) for a,b,c in zip(quarters(q_weight),quarters(k_weight),quarters(v_weight))]
    us=quarters(up_weight)
    own=jnp.stack([jnp.concatenate([a,b],1) for a,b in zip(qs,us)],1)
    full=lax.all_gather(own,"col",axis=1,tiled=True)
    turned=lax.all_to_all(full,"row",split_axis=1,concat_axis=0,tiled=True).reshape(D,-1)
    w_qkv=turned[:,0:576]; w_up=turned[:,576:]
    w_out=gather_col(out_weight); w_down=gather_col(down_weight)
    col=lambda vec,n:own_rows(vec,n,r)[:,None]
    g1,s1,g2,s2=[col(v,width) for v in (ln1_gain,ln1_bias,ln2_gain,ln2_bias)]
    bq=own_rows(q_bias,width,r); bv=own_rows(v_bias,width,r)
    b_qkv=head_order(bq,jnp.zeros_like(bq),bv)[:,None]
    b_out,b_down=col(out_bias,width),col(down_bias,width); b_up=col(up_bias,hidden)
    rel=rel_operands(rel_pos_h,rel_pos_w)
    x=tokens
    m,sq=row_stats(x,x*x)
    inv1=lax.rsqrt(sq-m*m+EPS); norm1=(x-m)*inv1
    a1=gather_rows((norm1*g1+s1).astype(bf16))
    qkv=(tn(w_qkv,a1)+b_qkv).astype(bf16)
    o=attend(offsets,qkv,rel)
    x1=x+sum_rows(lax.dot_general(w_out,o,(((0,),(1,)),((),())),preferred_element_type=f32))+b_out
    m2,sq2=row_stats(x1,x1*x1)
    inv2=lax.rsqrt(sq2-m2*m2+EPS); norm2=(x1-m2)*inv2
    a2=gather_rows((norm2*g2+s2).astype(bf16))
    h=tn(w_up,a2)+b_up
    act,slope=gelu_parts(h)
    g=act.astype(bf16)
    output=x1+sum_rows(tn(w_down,g))+b_down
    dy_own=cotangent.astype(bf16)
    dy=gather_rows(dy_own)
    d_down_bias=jnp.sum(dy_own,axis=1,dtype=f32)
    dh=(nn(w_down,dy)*slope).astype(bf16)
    d_down=nt(g,dy).astype(bf16)
    d_up=nt(a2,dh).astype(bf16)
    d_up_bias=jnp.sum(dh,axis=1,dtype=f32)
    da2=sum_rows(nn(w_up,dh))
    d_g2=jnp.sum(da2*norm2,axis=1); d_s2=jnp.sum(da2,axis=1)
    e2=da2*g2
    u,w=row_stats(e2,e2*norm2)
    dx1=cotangent+inv2*(e2-u-norm2*w)
    dat_own=dx1.astype(bf16)
    d_out_bias=jnp.sum(dat_own,axis=1,dtype=f32)
    dat=gather_rows(dat_own)
    d_out=lax.dot_general(o,dat,(((0,),(1,)),((),())),preferred_element_type=f32).astype(bf16)
    do=nn(w_out,dat).astype(bf16)
    dqkv,drel=attend_back(offsets,qkv,do,rel)
    d_qkv=nn(a1,dqkv).astype(bf16)
    b_sums=head_unorder(jnp.sum(dqkv,axis=0,dtype=f32))
    da1=sum_rows(nt(w_qkv,dqkv))
    d_g1=jnp.sum(da1*norm1,axis=1); d_s1=jnp.sum(da1,axis=1)
    e1=da1*g1
    u,w=row_stats(e1,e1*norm1)
    input_grad=dx1+inv1*(e1-u-norm1*w)
    def turn_back(dw):
        n=dw.shape[1]
        t=lax.all_to_all(dw.reshape(rows,width,n),"row",split_axis=0,concat_axis=0,tiled=True)
        return t
    def reduce(t,axis):
        return lax.psum(lax.psum_scatter(t,"col",scatter_dimension=axis,tiled=True),"dp").astype(f32)
    t_up=reduce(turn_back(d_up),0); t_qkv=reduce(turn_back(d_qkv),0)
    f_up=jnp.concatenate([t_up[i] for i in range(per)],1)
    parts=[head_unorder(t_qkv[i]) for i in range(per)]
    f_q,f_k,f_v=[jnp.concatenate([p[i] for p in parts],1) for i in range(3)]
    f_down=reduce(d_down,1); f_out=reduce(d_out,1)
    dh_rel,dw_rel=rel_grads(drel)
    minor=lax.psum((spread(d_g1,D,r),spread(d_s1,D,r),spread(b_sums[0],D,r),spread(b_sums[2],D,r),dh_rel,dw_rel,
      spread(d_out_bias,D,r),spread(d_g2,D,r),spread(d_s2,D,r),spread(d_up_bias,up_bias.shape[0],r),spread(d_down_bias,D,r)),("dp","row","col"))
    return (output,input_grad,minor[0],minor[1],f_q,f_k,f_v,minor[2],minor[3],minor[4],minor[5],f_out,minor[6],minor[7],
            minor[8],f_up,minor[9],f_down,minor[10])

def solution(mesh):
    act=P("row",("dp","col")); mat=P("row","col"); rep=P()
    return jax.shard_map(local,mesh=mesh,
      in_specs=(act,act,P(("dp","col"),None),rep,rep,mat,mat,mat,rep,rep,rep,rep,mat,rep,rep,rep,mat,rep,mat,rep),
      out_specs=(act,act,rep,rep,mat,mat,mat,rep,rep,rep,rep,mat,rep,rep,rep,mat,rep,mat,rep),check_vma=False)
```

```python
import functools
import jax, jax.numpy as jnp
from jax import lax
from jax.sharding import PartitionSpec as P
from jax.experimental import pallas as pl
from jax.experimental.pallas import tpu as pltpu

WIN=14; SIDE=32; CELL=16; GRIDW=48; PAD=10; NEG=-1e30
SLOTS=((0,128),(128,128),(256,128),(384,64),(448,64),(512,64))
f32=jnp.float32; bf16=jnp.bfloat16

def nt(a,b): return lax.dot_general(a,b,(((1,),(1,)),((),())),preferred_element_type=f32)
def nn(a,b): return lax.dot_general(a,b,(((1,),(0,)),((),())),preferred_element_type=f32)
def tn(a,b): return lax.dot_general(a,b,(((0,),(0,)),((),())),preferred_element_type=f32)

def codes():
    i=jnp.arange(8*GRIDW,dtype=jnp.int32); cell=i%GRIDW; xx=cell%CELL
    cells=jnp.where(xx<WIN,(i//GRIDW)*1000+(cell//CELL)*WIN+xx,-100000)
    j=jnp.arange(8*SIDE,dtype=jnp.int32)
    toks=(j//SIDE)*1000+j%SIDE
    return cells,toks

def rel_operands(rel_h,rel_w):
    h=rel_h[::-1].astype(bf16).T; w=rel_w[::-1].astype(bf16).T
    z=jnp.zeros((2,128,256),bf16)
    n=2*WIN-1
    z=z.at[0,0:64,64:64+n].set(h).at[0,0:64,128+65:128+65+n].set(w)
    z=z.at[1,64:128,0:n].set(h).at[1,64:128,128+1:128+1+n].set(w)
    return z

def spot_to_cells(slot_ref,src,cells_col,toks_row,c0):
    pass

def place(z,feat,spots,dmat,g):
    for row,width,lane in spots:
        got=nt(dmat,feat[row:row+width,256*g:256*(g+1)]).astype(bf16)
        z[pl.ds(PAD+8*g,8),:,lane:lane+width]=got.reshape(8,GRIDW,width)

def head_consts():
    lane=lax.broadcasted_iota(jnp.int32,(WIN,CELL,128),2)
    y=lax.broadcasted_iota(jnp.int32,(WIN,CELL,128),0)
    x=lax.broadcasted_iota(jnp.int32,(WIN,CELL,128),1)
    return lane,y,x

def skew(t,sign):
    th=t[:,0:128]; tw=t[:,128:256]
    outs=[]; outw=[]
    for y in range(WIN):
        a=th[CELL*y:CELL*(y+1)]
        s=(sign*(y-13))%128
        outs.append(pltpu.roll(a,s,1) if s else a)
        if sign>0:
            outw.append(pltpu.roll(tw[CELL*y:CELL*(y+1)],0,1,stride=1,stride_axis=0))
    if sign<0:
        x=lax.broadcasted_iota(jnp.int32,(WIN*CELL,128),0)&(CELL-1)
        for bit in (1,2,4,8):
            tw=jnp.where((x&bit)>0,pltpu.roll(tw,128-bit,1),tw)
        outw=[tw]
    return jnp.concatenate(outs,0),jnp.concatenate(outw,0)

def query_operand(q,rel,base,lane2,own):
    t=nn(q,rel)
    a,b=skew(t,1)
    in_h=(lane2>=base)&(lane2<base+WIN); in_w=(lane2>=base+WIN)&(lane2<base+2*WIN)
    both=jnp.where(in_h,a,jnp.where(in_w,b,0.0))
    hi=both.astype(bf16)
    lo=(both-hi.astype(f32)).astype(bf16)
    one=(lane2==base+2*WIN).astype(f32)
    first=(q.astype(f32)*0.125+hi.astype(f32)+one).astype(bf16)
    return jnp.concatenate([first,lo],1)

def key_operand(k,base,wy,wx,r0,c0):
    lane,y,x=head_consts()
    g=WIN*wy+y-r0; c=WIN*wx+x-c0
    ok=(g>=0)&(g<SIDE)&(c>=0)&(c<SIDE)&(x<WIN)
    eye=(((lane-base)==y)|((lane-base-WIN)==x)&(x<WIN)).astype(f32)
    eye=eye.reshape(WIN*CELL,128)
    mask=jnp.where((lane==base+2*WIN)&jnp.logical_not(ok),NEG,0.0).reshape(WIN*CELL,128)
    first=(k.astype(f32)+eye+mask).astype(bf16)
    return jnp.concatenate([first,eye.astype(bf16)],1)

HEADS3=((0,128*0,0),(1,128*0,0),(0,128*3,1))

def load_win(z,wy,wx,r0,lane):
    row=WIN*wy-r0+PAD
    return z[pl.ds(row,WIN),pl.ds(pl.multiple_of(CELL*wx,CELL),CELL),lane:lane+128].reshape(WIN*CELL,128)

def half_mask(v,half,lane2):
    keep=(lane2<64) if half==0 else (lane2>=64)
    return jnp.where(keep,v.astype(f32),0.0).astype(bf16)

def fwd_kernel(off,qkv,rel,cells,toks,o_ref,z,ow):
    r0=off[0,0]; c0=off[0,1]
    dmat=((cells[...]-c0)==toks[...]).astype(f32).astype(bf16)
    z[0:PAD]=jnp.zeros((PAD,GRIDW,768),bf16)
    z[PAD+SIDE:]=jnp.zeros((PAD,GRIDW,768),bf16)
    for lane in (384,512,640):
        z[PAD:PAD+SIDE,:,lane:lane+128]=jnp.zeros((SIDE,GRIDW,128),bf16)
    spots=[(r,w,128*i) for i,(r,w) in enumerate(SLOTS)]
    for g in range(4): place(z,qkv,spots,dmat,g)
    def window(n,carry):
        wy=n//3; wx=n%3
        lane2=lax.broadcasted_iota(jnp.int32,(WIN*CELL,128),1)
        for pair in range(2):
            q=load_win(z,wy,wx,r0,384*pair); k=load_win(z,wy,wx,r0,384*pair+128); v=load_win(z,wy,wx,r0,384*pair+256)
            total=None
            for half in range(2-pair):
                base=64 if half==0 else 0
                qq=half_mask(q,half,lane2); kk=half_mask(k,half,lane2)
                qc=query_operand(qq,rel[half],base,lane2,half)
                kc=key_operand(kk,base,wy,wx,r0,c0)
                s=nt(qc,kc)
                m=jnp.max(s,axis=1,keepdims=True)
                e=jnp.exp(s-m)
                p=(e*(1.0/jnp.sum(e,axis=1,keepdims=True))).astype(bf16)
                o=nn(p,v)
                total=o if total is None else jnp.where(lane2<64,total,o)
            ow[pl.ds(WIN*wy,WIN),pl.ds(pl.multiple_of(CELL*wx,CELL),CELL),128*pair:128*pair+128]=total.astype(bf16).reshape(WIN,CELL,128)
        return carry
    lax.fori_loop(0,9,window,0)
    for g in range(4):
        rows=ow[pl.ds(r0+8*g,8)].reshape(8*GRIDW,256)
        got=tn(dmat,rows)
        o_ref[256*g:256*(g+1),0:192]=got[:,0:192].astype(bf16)

def attend(off,qkv,rel):
    cells,toks=codes()
    return pl.pallas_call(fwd_kernel,out_shape=jax.ShapeDtypeStruct((1024,192),bf16),
      in_specs=[pl.BlockSpec(memory_space=pltpu.SMEM)]+[pl.BlockSpec(memory_space=pltpu.VMEM)]*4,
      out_specs=pl.BlockSpec(memory_space=pltpu.VMEM),
      scratch_shapes=[pltpu.VMEM((SIDE+2*PAD,GRIDW,768),bf16),pltpu.VMEM((42,GRIDW,256),bf16)],
      compiler_params=pltpu.CompilerParams(vmem_limit_bytes=56<<20),name="attend",
    )(off,qkv,rel,cells[:,None],toks[None,:])

def bwd_kernel(off,qkv,do,rel,cells,toks,g_ref,drel_ref,z,gw,tw):
    r0=off[0,0]; c0=off[0,1]
    dmat=((cells[...]-c0)==toks[...]).astype(f32).astype(bf16)
    z[0:PAD]=jnp.zeros((PAD,GRIDW,1024),bf16)
    z[PAD+SIDE:]=jnp.zeros((PAD,GRIDW,1024),bf16)
    for lane in (384,512,640,896):
        z[PAD:PAD+SIDE,:,lane:lane+128]=jnp.zeros((SIDE,GRIDW,128),bf16)
    spots=[(r,w,128*i) for i,(r,w) in enumerate(SLOTS)]
    for g in range(4):
        place(z,qkv,spots,dmat,g)
        place(z,do,((0,128,768),(128,64,896)),dmat,g)
    drel_ref[...]=jnp.zeros(drel_ref.shape,f32)
    def window(n,carry):
        wy=n//3; wx=n%3
        lane2=lax.broadcasted_iota(jnp.int32,(WIN*CELL,128),1)
        lane4=lax.broadcasted_iota(jnp.int32,(WIN*CELL,256),1)
        for pair in range(2):
            q=load_win(z,wy,wx,r0,384*pair); k=load_win(z,wy,wx,r0,384*pair+128); v=load_win(z,wy,wx,r0,384*pair+256)
            d=load_win(z,wy,wx,r0,768+128*pair)
            dq=dk=dv=None
            for half in range(2-pair):
                base=64 if half==0 else 0
                qq=half_mask(q,half,lane2); kk=half_mask(k,half,lane2); dd=half_mask(d,half,lane2)
                qc=query_operand(qq,rel[half],base,lane2,half)
                kc=key_operand(kk,base,wy,wx,r0,c0)
                s=nt(qc,kc)
                m=jnp.max(s,axis=1,keepdims=True)
                e=jnp.exp(s-m)
                p=e*(1.0/jnp.sum(e,axis=1,keepdims=True))
                pb=p.astype(bf16)
                dp=nt(dd,v)
                centre=jnp.sum(p*dp,axis=1,keepdims=True)
                ds=(p*(dp-centre)).astype(bf16)
                dvh=tn(pb,dd)
                dkh=tn(ds,qq)*0.125
                dqc=nn(ds,kc[:,0:128])
                t=jnp.concatenate([jnp.where((lane2>=base)&(lane2<base+WIN),dqc,0.0),
                                   jnp.where((lane2>=base+WIN)&(lane2<base+2*WIN),dqc,0.0)],1)
                a,b=skew(t,-1)
                t=jnp.concatenate([a,b],1)
                thi=t.astype(bf16)
                tlo=(t-thi.astype(f32)).astype(bf16)
                own=(lane2<64) if half==0 else (lane2>=64)
                dqh=jnp.where(own,dqc*0.125,0.0)+nt(thi,rel[half])+nt(tlo,rel[half])
                drel_ref[half]+=tn(qq,thi)
                if dq is None: dq,dk,dv=dqh,dkh,dvh
                else: dq,dk,dv=dq+dqh,dk+dkh,dv+dvh
            rows=pl.ds(WIN*wy,WIN); cols=pl.ds(pl.multiple_of(CELL*wx,CELL),CELL)
            for i,val in enumerate((dq,dk,dv)):
                lane=384*pair+128*i
                gw[rows,cols,lane:lane+128]=val.astype(bf16).reshape(WIN,CELL,128)
        return carry
    lax.fori_loop(0,9,window,0)
    for g in range(4):
        for i,(r,w) in enumerate(SLOTS):
            rows=gw[pl.ds(r0+8*g,8),:,128*i:128*i+128].reshape(8*GRIDW,128)
            got=tn(dmat,rows)
            g_ref[256*g:256*(g+1),r:r+w]=got[:,0:w].astype(bf16)

def attend_back(off,qkv,do,rel):
    cells,toks=codes()
    return pl.pallas_call(bwd_kernel,out_shape=(jax.ShapeDtypeStruct((1024,576),bf16),jax.ShapeDtypeStruct((2,128,256),f32)),
      in_specs=[pl.BlockSpec(memory_space=pltpu.SMEM)]+[pl.BlockSpec(memory_space=pltpu.VMEM)]*5,
      out_specs=(pl.BlockSpec(memory_space=pltpu.VMEM),)*2,
      scratch_shapes=[pltpu.VMEM((SIDE+2*PAD,GRIDW,1024),bf16),pltpu.VMEM((42,GRIDW,768),bf16),pltpu.VMEM((8,128),f32)],
      compiler_params=pltpu.CompilerParams(vmem_limit_bytes=56<<20),name="attend_back",
    )(off,qkv,do,rel,cells[:,None],toks[None,:])

def rel_grads(drel):
    n=2*WIN-1
    h=drel[0,0:64,64:64+n]+drel[1,64:128,0:n]
    w=drel[0,0:64,193:193+n]+drel[1,64:128,129:129+n]
    return h.T[::-1],w.T[::-1]

EPS=1e-06
D=768

def gelu_parts(h):
    cdf=0.5*(1.0+lax.erf(h*0.7071067811865476))
    pdf=jnp.exp(-0.5*h*h)*0.3989422804014327
    return h*cdf,cdf+h*pdf

def own_rows(vector,length,place):
    return lax.dynamic_slice_in_dim(vector,place*length,length,0)

def spread(portion,whole,place):
    return lax.dynamic_update_slice_in_dim(jnp.zeros((whole,),f32),portion,place*portion.shape[0],0)

def head_order(q,k,v):
    return jnp.concatenate([q[...,0:128],k[...,0:128],v[...,0:128],q[...,128:],k[...,128:],v[...,128:]],-1)

def head_unorder(m):
    cat=lambda a,b:jnp.concatenate([m[...,a:a+128],m[...,b:b+64]],-1)
    return cat(0,384),cat(128,448),cat(256,512)

def gather_rows(block):
    return lax.all_gather(block,"row",axis=0,tiled=True)

def sum_rows(partial):
    return lax.psum_scatter(partial.astype(bf16),"row",scatter_dimension=0,tiled=True).astype(f32)

def row_stats(*vals):
    both=lax.psum(jnp.stack([jnp.sum(v,axis=0) for v in vals]),"row")
    return [both[i:i+1]/D for i in range(len(vals))]


CH=4
VM=pl.BlockSpec(memory_space=pltpu.VMEM)
SEM=pltpu.SemaphoreType.DMA

class Row:
    def __init__(self):
        self.me=lax.axis_index("row")
        self.near=self.me+1-2*lax.rem(self.me,2)
        self.far=lax.rem(self.me+2,4)
        self.both=lax.rem(self.near+2,4)

def send(src,dst,ssem,rsem,row,col=None):
    where={"row":row} if col is None else {"row":row,"col":col}
    return pltpu.make_async_remote_copy(src_ref=src,dst_ref=dst,send_sem=ssem,recv_sem=rsem,device_id=where,device_id_type=pl.DeviceIdType.MESH)

def greet_row(p):
    sem=pltpu.get_barrier_semaphore()
    for peer in (p.near,p.far,p.both):
        pl.semaphore_signal(sem,inc=1,device_id={"row":peer},device_id_type=pl.DeviceIdType.MESH)
    pl.semaphore_wait(sem,3)

class Gather:
    def __init__(self,p,buf,sems,use):
        self.p,self.buf,self.sems,self.use,self.flight=p,buf,sems,use,{}
    def rows(self,t,b):
        n=self.buf.shape[1]//4
        return self.buf.at[t,pl.ds(pl.multiple_of(b*n,n),n)]
    def start(self,t,value):
        n=self.buf.shape[1]//4; p=self.p
        self.buf[t,pl.ds(pl.multiple_of(p.me*n,n),n)]=value
        mine=self.rows(t,p.me); s=lambda k:self.sems.at[self.use,t,k]
        far=send(mine,mine,s(0),s(1),p.far); near=send(mine,mine,s(2),s(3),p.near)
        far.start(); near.start()
        self.flight[t]=[far,near]
    def forward(self,t):
        p=self.p; s=lambda k:self.sems.at[self.use,t,k]
        self.flight[t][0].wait_recv()
        got=self.rows(t,p.far)
        on=send(got,got,s(4),s(5),p.near)
        on.start(); self.flight[t].append(on)
    def wait(self,t):
        self.flight[t][1].wait_recv(); self.flight[t][2].wait_recv()
        return self.buf[t]
    def drain(self):
        for copies in self.flight.values():
            for c in copies: c.wait_send()

class Scatter:
    def __init__(self,p,part,s1,r1,s2,r2,sems,use):
        self.p,self.part,self.s1,self.r1,self.s2,self.r2,self.sems,self.use,self.flight=p,part,s1,r1,s2,r2,sems,use,{}
    def block(self,t,b):
        n=self.part.shape[1]//4
        return self.part[t,pl.ds(pl.multiple_of(b*n,n),n)]
    def start(self,t):
        p=self.p; u=self.use
        self.s1[u,t,0]=self.block(t,p.near).astype(bf16)
        self.s1[u,t,1]=self.block(t,p.both).astype(bf16)
        c=send(self.s1.at[u,t],self.r1.at[u,t],self.sems.at[u,t,0],self.sems.at[u,t,1],p.near)
        c.start(); self.flight[t]=[c]
    def cross(self,t):
        p=self.p; u=self.use
        self.flight[t][0].wait_recv()
        self.s2[u,t]=(self.block(t,p.far)+self.r1[u,t,1].astype(f32)).astype(bf16)
        c=send(self.s2.at[u,t],self.r2.at[u,t],self.sems.at[u,t,2],self.sems.at[u,t,3],p.far)
        c.start(); self.flight[t].append(c)
    def wait(self,t):
        u=self.use
        self.flight[t][1].wait_recv()
        return self.block(t,self.p.me)+self.r1[u,t,0].astype(f32)+self.r2[u,t].astype(f32)
    def drain(self):
        for copies in self.flight.values():
            for c in copies: c.wait_send()

class Totals:
    def __init__(self,p,out,got,sems,use):
        self.p,self.out,self.got,self.sems,self.use,self.flight=p,out,got,sems,use,{}
    def start(self,t,a,b):
        u=self.use; p=self.p
        self.out[u,t,0:1]=jnp.sum(a,axis=0,keepdims=True)
        self.out[u,t,1:2]=jnp.sum(b,axis=0,keepdims=True)
        copies=[]
        for i,peer in enumerate((p.near,p.far,p.both)):
            c=send(self.out.at[u,t],self.got.at[u,t,i],self.sems.at[u,t,2*i],self.sems.at[u,t,2*i+1],peer)
            c.start(); copies.append(c)
        self.flight[t]=copies
    def wait(self,t):
        u=self.use
        for c in self.flight[t]: c.wait_recv()
        total=self.out[u,t]+self.got[u,t,0]+self.got[u,t,1]+self.got[u,t,2]
        return total[0:1]/D,total[1:2]/D
    def drain(self):
        for copies in self.flight.values():
            for c in copies: c.wait_send()

def tiled(rows,step,body):
    def run(i,carry):
        body(pl.ds(pl.multiple_of(i*step,step),step))
        return carry
    lax.fori_loop(0,rows//step,run,0)

def turn(dst,src):
    m,n=src.shape
    step=128 if m%128==0 else 64
    for i in range(0,m,step):
        dst[:,i:i+step]=src[i:i+step,:].T

def mlp_kernel(x_ref,cot_ref,o_ref,wo,wu,wd,bo,g2,s2,bu,bd,
               y_ref,dx1_ref,do_ref,dwo_ref,dwd_ref,dwu_ref,dg2_ref,ds2_ref,dbo_ref,dbd_ref,dbu_ref,
               wot,wut,wdt,part,part2,a2,dyb,dat,gb,dhb,x1b,st,da2b,s1b,r1b,s2b,r2b,tout,tgot,gsem,ssem,tsem):
    p=Row(); T=x_ref.shape[1]//CH
    cols=lambda t:slice(T*t,T*(t+1))
    greet_row(p)
    out_sum=Scatter(p,part,s1b,r1b,s2b,r2b,ssem,0)
    y_sum=Scatter(p,part2,s1b,r1b,s2b,r2b,ssem,1)
    da_sum=Scatter(p,part,s1b,r1b,s2b,r2b,ssem,2)
    ga,gy,gd=[Gather(p,b,gsem,i) for i,b in enumerate((a2,dyb,dat))]
    st2,stb=Totals(p,tout,tgot,tsem,0),Totals(p,tout,tgot,tsem,1)
    turn(wot,wo)
    def project(t):
        part[t]=nt(wot[...],o_ref[T*t:T*(t+1),:])
        out_sum.start(t)
    def residual(t):
        x1=x_ref[:,cols(t)]+out_sum.wait(t)+bo[...]
        x1b[t]=x1
        st2.start(t,x1,x1*x1)
    def second_norm(t):
        m,sq=st2.wait(t)
        inv=lax.rsqrt(sq-m*m+EPS)
        st[t,0:1]=m; st[t,1:2]=inv
        ga.start(t,((x1b[t]-m)*inv*g2[...]+s2[...]).astype(bf16))
        gy.start(t,cot_ref[:,cols(t)].astype(bf16))
    def hidden(t):
        ga.wait(t); gy.wait(t)
        def tile(r):
            h=nn(wut[r,:],a2[t])+bu[r,:]
            act,slope=gelu_parts(h)
            gb[t,r]=act.astype(bf16)
            dh=(nn(wd[r,:],dyb[t])*slope).astype(bf16)
            dhb[t,r]=dh
            dbu_ref[r,:]+=jnp.sum(dh.astype(f32),axis=1,keepdims=True)
        tiled(wut.shape[0],128,tile)
        def back(r):
            part[t,r]=nn(wu[r,:],dhb[t])
        tiled(wu.shape[0],256,back)
        da_sum.start(t)
    def down(t):
        def tile(r):
            part2[t,r]=nn(wdt[r,:],gb[t])
        tiled(wdt.shape[0],256,tile)
        y_sum.start(t)
    def norm_of(t): return (x1b[t]-st[t,0:1])*st[t,1:2]
    def second_back(t):
        da2=da_sum.wait(t); norm=norm_of(t)
        dg2_ref[...]+=jnp.sum(da2*norm,axis=1,keepdims=True)
        ds2_ref[...]+=jnp.sum(da2,axis=1,keepdims=True)
        e=da2*g2[...]
        da2b[t]=e
        stb.start(t,e,e*norm)
    def middle(t):
        u,w=stb.wait(t)
        dx1=cot_ref[:,cols(t)]+st[t,1:2]*(da2b[t]-u-norm_of(t)*w)
        dx1_ref[:,cols(t)]=dx1
        low=dx1.astype(bf16)
        dbo_ref[...]+=jnp.sum(low.astype(f32),axis=1,keepdims=True)
        gd.start(t,low)
    def attended(t):
        gd.wait(t)
        do_ref[:,cols(t)]=nn(wo[...],dat[t]).astype(bf16)
    def finish(t):
        y_ref[:,cols(t)]=x1b[t]+y_sum.wait(t)+bd[...]
    for ref in (dg2_ref,ds2_ref,dbo_ref,dbd_ref,dbu_ref): ref[...]=jnp.zeros(ref.shape,f32)
    def weight_grads():
        def one(r):
            acc=None; acc2=None
            for t in range(CH):
                v=nt(gb[t,r],dyb[t]); acc=v if acc is None else acc+v
                v=nt(a2[t,r],dhb[t]); acc2=v if acc2 is None else acc2+v
            dwd_ref[r,:]=acc.astype(bf16)
            dwu_ref[r,:]=acc2.astype(bf16)
        tiled(dwd_ref.shape[0],128,one)
    for t in range(CH): project(t)
    for t in range(CH): out_sum.cross(t)
    turn(wut,wu); turn(wdt,wd)
    for t in range(CH):
        residual(t)
        if t>0: second_norm(t-1)
    second_norm(CH-1)
    for t in range(CH):
        ga.forward(t); gy.forward(t)
        hidden(t)
        if t>0: da_sum.cross(t-1)
    down(0); da_sum.cross(CH-1)
    for t in range(1,CH): down(t)
    for t in range(CH):
        second_back(t)
        if t>0: middle(t-1)
    middle(CH-1)
    for t in range(CH): y_sum.cross(t)
    for t in range(CH): dbd_ref[...]+=jnp.sum(cot_ref[:,cols(t)].astype(bf16).astype(f32),axis=1,keepdims=True)
    for t in range(CH): gd.forward(t)
    weight_grads()
    for t in range(CH): attended(t)
    acc=None
    for t in range(CH):
        v=nt(o_ref[T*t:T*(t+1),:].T,dat[t]); acc=v if acc is None else acc+v
    dwo_ref[...]=acc.astype(bf16)
    for t in range(CH): finish(t)
    for c in (out_sum,y_sum,da_sum,ga,gy,gd,st2,stb): c.drain()

def mlp_block(x,cot,o,wo,wu,wd,bo,g2,s2,bu,bd):
    w,n=x.shape; T=n//CH; hid=wu.shape[1]; d=wu.shape[0]
    sd=jax.ShapeDtypeStruct; V=pltpu.VMEM
    return pl.pallas_call(mlp_kernel,name="mlp_block",
      out_shape=(sd((w,n),f32),sd((w,n),f32),sd((w,n),bf16),sd(wo.shape,bf16),sd((hid,d),bf16),sd((d,hid),bf16),
                 sd((w,1),f32),sd((w,1),f32),sd((w,1),f32),sd((w,1),f32),sd((hid,1),f32)),
      in_specs=[VM]*11,out_specs=(VM,)*11,
      scratch_shapes=[V((d,w),bf16),V((hid,d),bf16),V((d,hid),bf16),V((CH,d,T),f32),V((CH,d,T),f32),
        V((CH,d,T),bf16),V((CH,d,T),bf16),V((CH,d,T),bf16),V((CH,hid,T),bf16),V((CH,hid,T),bf16),
        V((CH,w,T),f32),V((CH,8,T),f32),V((CH,w,T),f32),
        V((3,CH,2,w,T),bf16),V((3,CH,2,w,T),bf16),V((3,CH,w,T),bf16),V((3,CH,w,T),bf16),
        V((2,CH,8,T),f32),V((2,CH,3,8,T),f32),SEM((3,CH,6)),SEM((3,CH,4)),SEM((2,CH,6))],
      cost_estimate=pl.CostEstimate(flops=8*10**9,bytes_accessed=3*10**7,transcendentals=10**6),
      compiler_params=pltpu.CompilerParams(collective_id=1,has_side_effects=True,vmem_limit_bytes=60<<20),
    )(x,cot,o,wo,wu,wd,bo,g2,s2,bu,bd)

def local(tokens,cotangent,offsets,ln1_gain,ln1_bias,q_weight,k_weight,v_weight,q_bias,v_bias,rel_pos_h,rel_pos_w,
          out_weight,out_bias,ln2_gain,ln2_bias,up_weight,up_bias,down_weight,down_bias):
    rows=lax.axis_size("row"); r=lax.axis_index("row"); cols=lax.axis_size("col")
    width=tokens.shape[0]; hidden=up_bias.shape[0]//rows
    gather_col=lambda w:lax.all_gather(w.astype(bf16),"col",axis=1,tiled=True)
    per=rows//cols
    def quarters(w):
        n=w.shape[1]//per
        return [w[:,n*i:n*i+n].astype(bf16) for i in range(per)]
    qs=[head_order(a,b,c) for a,b,c in zip(quarters(q_weight),quarters(k_weight),quarters(v_weight))]
    us=quarters(up_weight)
    own=jnp.stack([jnp.concatenate([a,b],1) for a,b in zip(qs,us)],1)
    full=lax.all_gather(own,"col",axis=1,tiled=True)
    turned=lax.all_to_all(full,"row",split_axis=1,concat_axis=0,tiled=True).reshape(D,-1)
    w_qkv=turned[:,0:576]; w_up=turned[:,576:]
    w_out=gather_col(out_weight); w_down=gather_col(down_weight)
    col=lambda vec,n:own_rows(vec,n,r)[:,None]
    g1,s1,g2,s2=[col(v,width) for v in (ln1_gain,ln1_bias,ln2_gain,ln2_bias)]
    bq=own_rows(q_bias,width,r); bv=own_rows(v_bias,width,r)
    b_qkv=head_order(bq,jnp.zeros_like(bq),bv)[:,None]
    b_out,b_down=col(out_bias,width),col(down_bias,width); b_up=col(up_bias,hidden)
    rel=rel_operands(rel_pos_h,rel_pos_w)
    x=tokens
    m,sq=row_stats(x,x*x)
    inv1=lax.rsqrt(sq-m*m+EPS); norm1=(x-m)*inv1
    a1=gather_rows((norm1*g1+s1).astype(bf16))
    qkv=(tn(w_qkv,a1)+b_qkv).astype(bf16)
    o=attend(offsets,qkv,rel)
    output,dx1,do,d_out,d_down,d_up,d_g2,d_s2,d_out_bias,d_down_bias,d_up_bias=mlp_block(
        x,cotangent,o,w_out,w_up,w_down,b_out,g2,s2,b_up,b_down)
    d_g2,d_s2,d_out_bias,d_down_bias,d_up_bias=[v[:,0] for v in (d_g2,d_s2,d_out_bias,d_down_bias,d_up_bias)]
    dqkv,drel=attend_back(offsets,qkv,do,rel)
    d_qkv=nn(a1,dqkv).astype(bf16)
    b_sums=head_unorder(jnp.sum(dqkv,axis=0,dtype=f32))
    da1=sum_rows(nt(w_qkv,dqkv))
    d_g1=jnp.sum(da1*norm1,axis=1); d_s1=jnp.sum(da1,axis=1)
    e1=da1*g1
    u,w=row_stats(e1,e1*norm1)
    input_grad=dx1+inv1*(e1-u-norm1*w)
    def turn_back(dw):
        n=dw.shape[1]
        t=lax.all_to_all(dw.reshape(rows,width,n),"row",split_axis=0,concat_axis=0,tiled=True)
        return t
    def reduce(t,axis):
        return lax.psum(lax.psum_scatter(t,"col",scatter_dimension=axis,tiled=True),"dp").astype(f32)
    t_up=reduce(turn_back(d_up),0); t_qkv=reduce(turn_back(d_qkv),0)
    f_up=jnp.concatenate([t_up[i] for i in range(per)],1)
    parts=[head_unorder(t_qkv[i]) for i in range(per)]
    f_q,f_k,f_v=[jnp.concatenate([p[i] for p in parts],1) for i in range(3)]
    f_down=reduce(d_down,1); f_out=reduce(d_out,1)
    dh_rel,dw_rel=rel_grads(drel)
    minor=lax.psum((spread(d_g1,D,r),spread(d_s1,D,r),spread(b_sums[0],D,r),spread(b_sums[2],D,r),dh_rel,dw_rel,
      spread(d_out_bias,D,r),spread(d_g2,D,r),spread(d_s2,D,r),spread(d_up_bias,up_bias.shape[0],r),spread(d_down_bias,D,r)),("dp","row","col"))
    return (output,input_grad,minor[0],minor[1],f_q,f_k,f_v,minor[2],minor[3],minor[4],minor[5],f_out,minor[6],minor[7],
            minor[8],f_up,minor[9],f_down,minor[10])

def solution(mesh):
    act=P("row",("dp","col")); mat=P("row","col"); rep=P()
    return jax.shard_map(local,mesh=mesh,
      in_specs=(act,act,P(("dp","col"),None),rep,rep,mat,mat,mat,rep,rep,rep,rep,mat,rep,rep,rep,mat,rep,mat,rep),
      out_specs=(act,act,rep,rep,mat,mat,mat,rep,rep,rep,rep,mat,rep,rep,rep,mat,rep,mat,rep),check_vma=False)
```

```python
import functools
import jax, jax.numpy as jnp
from jax import lax
from jax.sharding import PartitionSpec as P
from jax.experimental import pallas as pl
from jax.experimental.pallas import tpu as pltpu

WIN=14; SIDE=32; CELL=16; GRIDW=48; PAD=10; NEG=-1e30
SLOTS=((0,128),(128,128),(256,128),(384,64),(448,64),(512,64))
f32=jnp.float32; bf16=jnp.bfloat16

def nt(a,b): return lax.dot_general(a,b,(((1,),(1,)),((),())),preferred_element_type=f32)
def nn(a,b): return lax.dot_general(a,b,(((1,),(0,)),((),())),preferred_element_type=f32)
def tn(a,b): return lax.dot_general(a,b,(((0,),(0,)),((),())),preferred_element_type=f32)

def codes():
    i=jnp.arange(8*GRIDW,dtype=jnp.int32); cell=i%GRIDW; xx=cell%CELL
    cells=jnp.where(xx<WIN,(i//GRIDW)*1000+(cell//CELL)*WIN+xx,-100000)
    j=jnp.arange(8*SIDE,dtype=jnp.int32)
    toks=(j//SIDE)*1000+j%SIDE
    return cells,toks

def rel_operands(rel_h,rel_w):
    h=rel_h[::-1].astype(bf16).T; w=rel_w[::-1].astype(bf16).T
    z=jnp.zeros((2,128,256),bf16)
    n=2*WIN-1
    z=z.at[0,0:64,64:64+n].set(h).at[0,0:64,128+65:128+65+n].set(w)
    z=z.at[1,64:128,0:n].set(h).at[1,64:128,128+1:128+1+n].set(w)
    return z

def spot_to_cells(slot_ref,src,cells_col,toks_row,c0):
    pass

def place(z,feat,spots,dmat,g):
    for row,width,lane in spots:
        got=nt(dmat,feat[row:row+width,256*g:256*(g+1)]).astype(bf16)
        z[pl.ds(PAD+8*g,8),:,lane:lane+width]=got.reshape(8,GRIDW,width)

def head_consts():
    lane=lax.broadcasted_iota(jnp.int32,(WIN,CELL,128),2)
    y=lax.broadcasted_iota(jnp.int32,(WIN,CELL,128),0)
    x=lax.broadcasted_iota(jnp.int32,(WIN,CELL,128),1)
    return lane,y,x

def skew(t,sign):
    th=t[:,0:128]; tw=t[:,128:256]
    outs=[]; outw=[]
    for y in range(WIN):
        a=th[CELL*y:CELL*(y+1)]
        s=(sign*(y-13))%128
        outs.append(pltpu.roll(a,s,1) if s else a)
        if sign>0:
            outw.append(pltpu.roll(tw[CELL*y:CELL*(y+1)],0,1,stride=1,stride_axis=0))
    if sign<0:
        x=lax.broadcasted_iota(jnp.int32,(WIN*CELL,128),0)&(CELL-1)
        for bit in (1,2,4,8):
            tw=jnp.where((x&bit)>0,pltpu.roll(tw,128-bit,1),tw)
        outw=[tw]
    return jnp.concatenate(outs,0),jnp.concatenate(outw,0)

def query_operand(q,rel,base,lane2,own):
    t=nn(q,rel)
    a,b=skew(t,1)
    in_h=(lane2>=base)&(lane2<base+WIN); in_w=(lane2>=base+WIN)&(lane2<base+2*WIN)
    both=jnp.where(in_h,a,jnp.where(in_w,b,0.0))
    hi=both.astype(bf16)
    lo=(both-hi.astype(f32)).astype(bf16)
    one=(lane2==base+2*WIN).astype(f32)
    first=(q.astype(f32)*0.125+hi.astype(f32)+one).astype(bf16)
    return jnp.concatenate([first,lo],1)

def key_operand(k,base,wy,wx,r0,c0):
    lane,y,x=head_consts()
    g=WIN*wy+y-r0; c=WIN*wx+x-c0
    ok=(g>=0)&(g<SIDE)&(c>=0)&(c<SIDE)&(x<WIN)
    eye=(((lane-base)==y)|((lane-base-WIN)==x)&(x<WIN)).astype(f32)
    eye=eye.reshape(WIN*CELL,128)
    mask=jnp.where((lane==base+2*WIN)&jnp.logical_not(ok),NEG,0.0).reshape(WIN*CELL,128)
    first=(k.astype(f32)+eye+mask).astype(bf16)
    return jnp.concatenate([first,eye.astype(bf16)],1)

HEADS3=((0,128*0,0),(1,128*0,0),(0,128*3,1))

def load_win(z,wy,wx,r0,lane):
    row=WIN*wy-r0+PAD
    return z[pl.ds(row,WIN),pl.ds(pl.multiple_of(CELL*wx,CELL),CELL),lane:lane+128].reshape(WIN*CELL,128)

def half_mask(v,half,lane2):
    keep=(lane2<64) if half==0 else (lane2>=64)
    return jnp.where(keep,v.astype(f32),0.0).astype(bf16)

def fwd_kernel(off,qkv,rel,cells,toks,o_ref,z,ow):
    r0=off[0,0]; c0=off[0,1]
    dmat=((cells[...]-c0)==toks[...]).astype(f32).astype(bf16)
    z[0:PAD]=jnp.zeros((PAD,GRIDW,768),bf16)
    z[PAD+SIDE:]=jnp.zeros((PAD,GRIDW,768),bf16)
    for lane in (384,512,640):
        z[PAD:PAD+SIDE,:,lane:lane+128]=jnp.zeros((SIDE,GRIDW,128),bf16)
    spots=[(r,w,128*i) for i,(r,w) in enumerate(SLOTS)]
    for g in range(4): place(z,qkv,spots,dmat,g)
    def window(n,carry):
        wy=n//3; wx=n%3
        lane2=lax.broadcasted_iota(jnp.int32,(WIN*CELL,128),1)
        for pair in range(2):
            q=load_win(z,wy,wx,r0,384*pair); k=load_win(z,wy,wx,r0,384*pair+128); v=load_win(z,wy,wx,r0,384*pair+256)
            total=None
            for half in range(2-pair):
                base=64 if half==0 else 0
                qq=half_mask(q,half,lane2); kk=half_mask(k,half,lane2)
                qc=query_operand(qq,rel[half],base,lane2,half)
                kc=key_operand(kk,base,wy,wx,r0,c0)
                s=nt(qc,kc)
                m=jnp.max(s,axis=1,keepdims=True)
                e=jnp.exp(s-m)
                p=(e*(1.0/jnp.sum(e,axis=1,keepdims=True))).astype(bf16)
                o=nn(p,v)
                total=o if total is None else jnp.where(lane2<64,total,o)
            ow[pl.ds(WIN*wy,WIN),pl.ds(pl.multiple_of(CELL*wx,CELL),CELL),128*pair:128*pair+128]=total.astype(bf16).reshape(WIN,CELL,128)
        return carry
    lax.fori_loop(0,9,window,0)
    for g in range(4):
        rows=ow[pl.ds(r0+8*g,8)].reshape(8*GRIDW,256)
        got=tn(dmat,rows)
        o_ref[256*g:256*(g+1),0:192]=got[:,0:192].astype(bf16)

def attend(off,qkv,rel):
    cells,toks=codes()
    return pl.pallas_call(fwd_kernel,out_shape=jax.ShapeDtypeStruct((1024,192),bf16),
      in_specs=[pl.BlockSpec(memory_space=pltpu.SMEM)]+[pl.BlockSpec(memory_space=pltpu.VMEM)]*4,
      out_specs=pl.BlockSpec(memory_space=pltpu.VMEM),
      scratch_shapes=[pltpu.VMEM((SIDE+2*PAD,GRIDW,768),bf16),pltpu.VMEM((42,GRIDW,256),bf16)],
      compiler_params=pltpu.CompilerParams(vmem_limit_bytes=56<<20),name="attend",
    )(off,qkv,rel,cells[:,None],toks[None,:])

def bwd_kernel(off,qkv,do,rel,cells,toks,g_ref,drel_ref,z,gw,tw):
    r0=off[0,0]; c0=off[0,1]
    dmat=((cells[...]-c0)==toks[...]).astype(f32).astype(bf16)
    z[0:PAD]=jnp.zeros((PAD,GRIDW,1024),bf16)
    z[PAD+SIDE:]=jnp.zeros((PAD,GRIDW,1024),bf16)
    for lane in (384,512,640,896):
        z[PAD:PAD+SIDE,:,lane:lane+128]=jnp.zeros((SIDE,GRIDW,128),bf16)
    spots=[(r,w,128*i) for i,(r,w) in enumerate(SLOTS)]
    for g in range(4):
        place(z,qkv,spots,dmat,g)
        place(z,do,((0,128,768),(128,64,896)),dmat,g)
    drel_ref[...]=jnp.zeros(drel_ref.shape,f32)
    def window(n,carry):
        wy=n//3; wx=n%3
        lane2=lax.broadcasted_iota(jnp.int32,(WIN*CELL,128),1)
        lane4=lax.broadcasted_iota(jnp.int32,(WIN*CELL,256),1)
        for pair in range(2):
            q=load_win(z,wy,wx,r0,384*pair); k=load_win(z,wy,wx,r0,384*pair+128); v=load_win(z,wy,wx,r0,384*pair+256)
            d=load_win(z,wy,wx,r0,768+128*pair)
            dq=dk=dv=None
            for half in range(2-pair):
                base=64 if half==0 else 0
                qq=half_mask(q,half,lane2); kk=half_mask(k,half,lane2); dd=half_mask(d,half,lane2)
                qc=query_operand(qq,rel[half],base,lane2,half)
                kc=key_operand(kk,base,wy,wx,r0,c0)
                s=nt(qc,kc)
                m=jnp.max(s,axis=1,keepdims=True)
                e=jnp.exp(s-m)
                p=e*(1.0/jnp.sum(e,axis=1,keepdims=True))
                pb=p.astype(bf16)
                dp=nt(dd,v)
                centre=jnp.sum(p*dp,axis=1,keepdims=True)
                ds=(p*(dp-centre)).astype(bf16)
                dvh=tn(pb,dd)
                dkh=tn(ds,qq)*0.125
                dqc=nn(ds,kc[:,0:128])
                t=jnp.concatenate([jnp.where((lane2>=base)&(lane2<base+WIN),dqc,0.0),
                                   jnp.where((lane2>=base+WIN)&(lane2<base+2*WIN),dqc,0.0)],1)
                a,b=skew(t,-1)
                t=jnp.concatenate([a,b],1)
                thi=t.astype(bf16)
                tlo=(t-thi.astype(f32)).astype(bf16)
                own=(lane2<64) if half==0 else (lane2>=64)
                dqh=jnp.where(own,dqc*0.125,0.0)+nt(thi,rel[half])+nt(tlo,rel[half])
                drel_ref[half]+=tn(qq,thi)
                if dq is None: dq,dk,dv=dqh,dkh,dvh
                else: dq,dk,dv=dq+dqh,dk+dkh,dv+dvh
            rows=pl.ds(WIN*wy,WIN); cols=pl.ds(pl.multiple_of(CELL*wx,CELL),CELL)
            for i,val in enumerate((dq,dk,dv)):
                lane=384*pair+128*i
                gw[rows,cols,lane:lane+128]=val.astype(bf16).reshape(WIN,CELL,128)
        return carry
    lax.fori_loop(0,9,window,0)
    for g in range(4):
        for i,(r,w) in enumerate(SLOTS):
            rows=gw[pl.ds(r0+8*g,8),:,128*i:128*i+128].reshape(8*GRIDW,128)
            got=tn(dmat,rows)
            g_ref[256*g:256*(g+1),r:r+w]=got[:,0:w].astype(bf16)

def attend_back(off,qkv,do,rel):
    cells,toks=codes()
    return pl.pallas_call(bwd_kernel,out_shape=(jax.ShapeDtypeStruct((1024,576),bf16),jax.ShapeDtypeStruct((2,128,256),f32)),
      in_specs=[pl.BlockSpec(memory_space=pltpu.SMEM)]+[pl.BlockSpec(memory_space=pltpu.VMEM)]*5,
      out_specs=(pl.BlockSpec(memory_space=pltpu.VMEM),)*2,
      scratch_shapes=[pltpu.VMEM((SIDE+2*PAD,GRIDW,1024),bf16),pltpu.VMEM((42,GRIDW,768),bf16),pltpu.VMEM((8,128),f32)],
      compiler_params=pltpu.CompilerParams(vmem_limit_bytes=56<<20),name="attend_back",
    )(off,qkv,do,rel,cells[:,None],toks[None,:])

def rel_grads(drel):
    n=2*WIN-1
    h=drel[0,0:64,64:64+n]+drel[1,64:128,0:n]
    w=drel[0,0:64,193:193+n]+drel[1,64:128,129:129+n]
    return h.T[::-1],w.T[::-1]

EPS=1e-06
D=768

def gelu_parts(h):
    cdf=0.5*(1.0+lax.erf(h*0.7071067811865476))
    pdf=jnp.exp(-0.5*h*h)*0.3989422804014327
    return h*cdf,cdf+h*pdf

def own_rows(vector,length,place):
    return lax.dynamic_slice_in_dim(vector,place*length,length,0)

def spread(portion,whole,place):
    return lax.dynamic_update_slice_in_dim(jnp.zeros((whole,),f32),portion,place*portion.shape[0],0)

def head_order(q,k,v):
    return jnp.concatenate([q[...,0:128],k[...,0:128],v[...,0:128],q[...,128:],k[...,128:],v[...,128:]],-1)

def head_unorder(m):
    cat=lambda a,b:jnp.concatenate([m[...,a:a+128],m[...,b:b+64]],-1)
    return cat(0,384),cat(128,448),cat(256,512)

def gather_rows(block):
    return lax.all_gather(block,"row",axis=0,tiled=True)

def sum_rows(partial):
    return lax.psum_scatter(partial.astype(bf16),"row",scatter_dimension=0,tiled=True).astype(f32)

def row_stats(*vals):
    both=lax.psum(jnp.stack([jnp.sum(v,axis=0) for v in vals]),"row")
    return [both[i:i+1]/D for i in range(len(vals))]


CH=4
VM=pl.BlockSpec(memory_space=pltpu.VMEM)
SEM=pltpu.SemaphoreType.DMA

class Row:
    def __init__(self):
        self.me=lax.axis_index("row")
        self.near=self.me+1-2*lax.rem(self.me,2)
        self.far=lax.rem(self.me+2,4)
        self.both=lax.rem(self.near+2,4)

def send(src,dst,ssem,rsem,row,col=None):
    where={"row":row} if col is None else {"row":row,"col":col}
    return pltpu.make_async_remote_copy(src_ref=src,dst_ref=dst,send_sem=ssem,recv_sem=rsem,device_id=where,device_id_type=pl.DeviceIdType.MESH)

def greet_row(p):
    sem=pltpu.get_barrier_semaphore()
    for peer in (p.near,p.far,p.both):
        pl.semaphore_signal(sem,inc=1,device_id={"row":peer},device_id_type=pl.DeviceIdType.MESH)
    pl.semaphore_wait(sem,3)

class Gather:
    def __init__(self,p,buf,sems,use):
        self.p,self.buf,self.sems,self.use,self.flight=p,buf,sems,use,{}
    def rows(self,t,b):
        n=self.buf.shape[1]//4
        return self.buf.at[t,pl.ds(pl.multiple_of(b*n,n),n)]
    def start(self,t,value):
        n=self.buf.shape[1]//4; p=self.p
        self.buf[t,pl.ds(pl.multiple_of(p.me*n,n),n)]=value
        mine=self.rows(t,p.me); s=lambda k:self.sems.at[self.use,t,k]
        far=send(mine,mine,s(0),s(1),p.far); near=send(mine,mine,s(2),s(3),p.near)
        far.start(); near.start()
        self.flight[t]=[far,near]
    def forward(self,t):
        p=self.p; s=lambda k:self.sems.at[self.use,t,k]
        self.flight[t][0].wait_recv()
        got=self.rows(t,p.far)
        on=send(got,got,s(4),s(5),p.near)
        on.start(); self.flight[t].append(on)
    def wait(self,t):
        self.flight[t][1].wait_recv(); self.flight[t][2].wait_recv()
        return self.buf[t]
    def drain(self):
        for copies in self.flight.values():
            for c in copies: c.wait_send()

class Scatter:
    def __init__(self,p,part,s1,r1,s2,r2,sems,use):
        self.p,self.part,self.s1,self.r1,self.s2,self.r2,self.sems,self.use,self.flight=p,part,s1,r1,s2,r2,sems,use,{}
    def block(self,t,b):
        n=self.part.shape[1]//4
        return self.part[t,pl.ds(pl.multiple_of(b*n,n),n)]
    def start(self,t):
        p=self.p; u=self.use
        self.s1[u,t,0]=self.block(t,p.near).astype(bf16)
        self.s1[u,t,1]=self.block(t,p.both).astype(bf16)
        c=send(self.s1.at[u,t],self.r1.at[u,t],self.sems.at[u,t,0],self.sems.at[u,t,1],p.near)
        c.start(); self.flight[t]=[c]
    def cross(self,t):
        p=self.p; u=self.use
        self.flight[t][0].wait_recv()
        self.s2[u,t]=(self.block(t,p.far)+self.r1[u,t,1].astype(f32)).astype(bf16)
        c=send(self.s2.at[u,t],self.r2.at[u,t],self.sems.at[u,t,2],self.sems.at[u,t,3],p.far)
        c.start(); self.flight[t].append(c)
    def wait(self,t):
        u=self.use
        self.flight[t][1].wait_recv()
        return self.block(t,self.p.me)+self.r1[u,t,0].astype(f32)+self.r2[u,t].astype(f32)
    def drain(self):
        for copies in self.flight.values():
            for c in copies: c.wait_send()

class Totals:
    def __init__(self,p,out,got,sems,use):
        self.p,self.out,self.got,self.sems,self.use,self.flight=p,out,got,sems,use,{}
    def start(self,t,a,b):
        u=self.use; p=self.p
        self.out[u,t,0:1]=jnp.sum(a,axis=0,keepdims=True)
        self.out[u,t,1:2]=jnp.sum(b,axis=0,keepdims=True)
        copies=[]
        for i,peer in enumerate((p.near,p.far,p.both)):
            c=send(self.out.at[u,t],self.got.at[u,t,i],self.sems.at[u,t,2*i],self.sems.at[u,t,2*i+1],peer)
            c.start(); copies.append(c)
        self.flight[t]=copies
    def wait(self,t):
        u=self.use
        for c in self.flight[t]: c.wait_recv()
        total=self.out[u,t]+self.got[u,t,0]+self.got[u,t,1]+self.got[u,t,2]
        return total[0:1]/D,total[1:2]/D
    def drain(self):
        for copies in self.flight.values():
            for c in copies: c.wait_send()

class Turn:
    def __init__(self,p,src,dst,sems):
        n=src.shape[0]//4
        rows=lambda b:src.at[pl.ds(pl.multiple_of(b*n,n),n)]
        self.copies=[]
        for i,peer in enumerate((p.far,p.both,p.near)):
            c=send(rows(peer),dst.at[p.me],sems.at[2*i],sems.at[2*i+1],peer)
            c.start(); self.copies.append(c)
        self.own=pltpu.make_async_copy(rows(p.me),dst.at[p.me],sems.at[6])
        self.own.start()
    def wait(self):
        for c in self.copies: c.wait_recv()
        for c in self.copies: c.wait_send()
        self.own.wait()

def greet(others):
    sem=pltpu.get_barrier_semaphore()
    for where in others:
        pl.semaphore_signal(sem,inc=1,device_id=where,device_id_type=pl.DeviceIdType.MESH)
    pl.semaphore_wait(sem,len(others))

def head_kernel(ncol,x_ref,oq_ref,ou_ref,g1,s1,bq,a1,qkv_ref,wq,wu,st,wqt,tout,tgot,gsem,tsem,ssem,rsem):
    p=Row(); T=x_ref.shape[1]//CH; per=4//ncol
    c=lax.axis_index("col")
    cols=lambda t:slice(T*t,T*(t+1))
    greet([{"row":lax.rem(p.me+i,4),"col":lax.rem(c+j,ncol)} for i in range(4) for j in range(ncol) if i or j])
    def push(k,own,full):
        for j in range(per):
            row=per*c+j
            for dc in range(ncol):
                copy=send(own.at[j],full.at[p.me],ssem.at[k,j,dc],rsem.at[k,p.me],row,lax.rem(c+dc,ncol))
                if dc: copy.start()
                else:
                    pl.when(row!=p.me)(copy.start)
                    pl.when(row==p.me)(pltpu.make_async_copy(own.at[j],full.at[p.me],rsem.at[k,p.me]).start)
    def arrive(k,own,full):
        for s in range(4):
            mine=jnp.logical_and(p.me==s,c==s//per)
            local_copy=pltpu.make_async_copy(own.at[0],full.at[s],rsem.at[k,s])
            remote=send(own.at[0],full.at[s],ssem.at[k,0,0],rsem.at[k,s],lax.rem(p.me+1,4),c)
            pl.when(mine)(local_copy.wait)
            pl.when(jnp.logical_not(mine))(remote.wait_recv)
    def sent(k,own,full):
        for j in range(per):
            row=per*c+j
            for dc in range(ncol):
                copy=send(own.at[j],full.at[p.me],ssem.at[k,j,dc],rsem.at[k,p.me],row,lax.rem(c+dc,ncol))
                if dc: copy.wait_send()
                else: pl.when(row!=p.me)(copy.wait_send)
    push(0,oq_ref,wq)
    tot=Totals(p,tout,tgot,tsem,0); ga=Gather(p,a1,gsem,0)
    for t in range(CH):
        v=x_ref[:,cols(t)]
        tot.start(t,v,v*v)
    for t in range(CH):
        m,sq=tot.wait(t)
        inv=lax.rsqrt(sq-m*m+EPS)
        st[t,0:1]=m; st[t,1:2]=inv
        ga.start(t,((x_ref[:,cols(t)]-m)*inv*g1[...]+s1[...]).astype(bf16))
    push(1,ou_ref,wu)
    arrive(0,oq_ref,wq)
    n=wq.shape[1]
    for s in range(4): wqt[:,n*s:n*s+n]=wq[s].T
    for t in range(CH): ga.forward(t)
    for t in range(CH):
        ga.wait(t)
        def tile(r):
            qkv_ref[r,cols(t)]=(nn(wqt[r,:],a1[t])+bq[r,:]).astype(bf16)
        tiled(wqt.shape[0],192,tile)
    arrive(1,ou_ref,wu)
    sent(0,oq_ref,wq); sent(1,ou_ref,wu)
    for q in (tot,ga): q.drain()

def head_block(x,oq,ou,g1,s1,bq,ncol):
    w,n=x.shape; T=n//CH; d=4*w; sd=jax.ShapeDtypeStruct; V=pltpu.VMEM
    nq=oq.shape[2]; per=4//ncol
    return pl.pallas_call(functools.partial(head_kernel,ncol),name="head_block",
      out_shape=(sd((CH,d,T),bf16),sd((nq,n),bf16),sd((4,w,nq),bf16),sd((4,w,ou.shape[2]),bf16),sd((CH,8,T),f32)),
      in_specs=[VM]*6,out_specs=(VM,)*5,
      scratch_shapes=[V((nq,d),bf16),V((1,CH,8,T),f32),V((1,CH,3,8,T),f32),SEM((1,CH,6)),SEM((1,CH,6)),SEM((2,per,ncol)),SEM((2,4))],
      cost_estimate=pl.CostEstimate(flops=10**9,bytes_accessed=10**8,transcendentals=0),
      compiler_params=pltpu.CompilerParams(collective_id=2,has_side_effects=True,vmem_limit_bytes=48<<20),
    )(x,oq,ou,g1,s1,bq)

def tail_kernel(ncol,dqkv,wq,a1,x_ref,st,dx1,g1,dwo,in_ref,q_out,o_out,dg1,ds1,
                part,s1b,r1b,s2b,r2b,tout,tgot,eb,dwq,tq,yq,yo,ssem,tsem,usem,ysem):
    p=Row(); T=x_ref.shape[1]//CH; per=4//ncol
    c=lax.axis_index("col"); other=ncol-1-c
    cols=lambda t:slice(T*t,T*(t+1))
    greet([{"row":q,"col":c} for q in (p.near,p.far,p.both)]+[{"row":p.me,"col":other}])
    half=dwo.shape[1]//ncol
    lanes=lambda k:pl.ds(pl.multiple_of(k*half,128),half)
    out_copy=send(dwo.at[:,lanes(other)],yo,ysem.at[0],ysem.at[1],p.me,other)
    out_copy.start()
    def grads(r):
        acc=None
        for t in range(CH):
            v=nn(a1[t,r],dqkv[T*t:T*(t+1),:]); acc=v if acc is None else acc+v
        dwq[r,:]=acc.astype(bf16)
    tiled(dwq.shape[0],192,grads)
    turned=Turn(p,dwq,tq,usem)
    total=Scatter(p,part,s1b,r1b,s2b,r2b,ssem,0); stats=Totals(p,tout,tgot,tsem,0)
    for t in range(CH):
        def tile(r):
            part[t,r]=nt(wq[r,:],dqkv[T*t:T*(t+1),:])
        tiled(wq.shape[0],192,tile)
        total.start(t)
        if t: total.cross(t-1)
    total.cross(CH-1)
    turned.wait()
    block=lambda k:tq.at[pl.ds(per*k,per)]
    q_copy=send(block(other),yq,ysem.at[2],ysem.at[3],p.me,other)
    q_copy.start()
    dg1[...]=jnp.zeros(dg1.shape,f32); ds1[...]=jnp.zeros(ds1.shape,f32)
    norm_of=lambda t:(x_ref[:,cols(t)]-st[t,0:1])*st[t,1:2]
    def first(t):
        da=total.wait(t); norm=norm_of(t)
        dg1[...]+=jnp.sum(da*norm,axis=1,keepdims=True)
        ds1[...]+=jnp.sum(da,axis=1,keepdims=True)
        e=da*g1[...]
        eb[t]=e
        stats.start(t,e,e*norm)
    def last(t):
        u,w=stats.wait(t)
        in_ref[:,cols(t)]=dx1[:,cols(t)]+st[t,1:2]*(eb[t]-u-norm_of(t)*w)
    for t in range(CH):
        first(t)
        if t: last(t-1)
    last(CH-1)
    out_copy.wait_recv()
    o_out[...]=(dwo[:,lanes(c)].astype(f32)+yo[...].astype(f32)).astype(bf16)
    q_copy.wait_recv()
    for i in range(per):
        q_out[i]=(tq[per*c+i].astype(f32)+yq[i].astype(f32)).astype(bf16)
    out_copy.wait_send(); q_copy.wait_send()
    for q in (total,stats): q.drain()

def tail_block(dqkv,wq,a1,x,st,dx1,g1,dwo,ncol):
    w,n=x.shape; T=n//CH; d=4*w; sd=jax.ShapeDtypeStruct; V=pltpu.VMEM
    nq=wq.shape[1]; per=4//ncol; half=dwo.shape[1]//ncol
    return pl.pallas_call(functools.partial(tail_kernel,ncol),name="tail_block",
      out_shape=(sd((w,n),f32),sd((per,w,nq),bf16),sd((w,half),bf16),sd((w,1),f32),sd((w,1),f32)),
      in_specs=[VM]*8,out_specs=(VM,)*5,
      scratch_shapes=[V((CH,d,T),f32),V((1,CH,2,w,T),bf16),V((1,CH,2,w,T),bf16),V((1,CH,w,T),bf16),V((1,CH,w,T),bf16),
        V((1,CH,8,T),f32),V((1,CH,3,8,T),f32),V((CH,w,T),f32),V((d,nq),bf16),V((4,w,nq),bf16),V((per,w,nq),bf16),V((w,half),bf16),
        SEM((1,CH,4)),SEM((1,CH,6)),SEM((7,)),SEM((4,))],
      cost_estimate=pl.CostEstimate(flops=2*10**9,bytes_accessed=10**8,transcendentals=0),
      compiler_params=pltpu.CompilerParams(collective_id=3,has_side_effects=True,vmem_limit_bytes=56<<20),
    )(dqkv,wq,a1,x,st,dx1,g1,dwo)

def tiled(rows,step,body):
    def run(i,carry):
        body(pl.ds(pl.multiple_of(i*step,step),step))
        return carry
    lax.fori_loop(0,rows//step,run,0)

def turn(dst,src):
    m,n=src.shape
    step=128 if m%128==0 else 64
    for i in range(0,m,step):
        dst[:,i:i+step]=src[i:i+step,:].T

def mlp_kernel(x_ref,cot_ref,o_ref,wo,wu,wd,bo,g2,s2,bu,bd,
               y_ref,dx1_ref,do_ref,dwo_ref,dwd_ref,tup_ref,dg2_ref,ds2_ref,dbo_ref,dbd_ref,dbu_ref,
               wot,wut,wdt,part,part2,a2,dyb,dat,gb,dhb,x1b,st,da2b,s1b,r1b,s2b,r2b,tout,tgot,dwu_ref,gsem,ssem,tsem,usem):
    p=Row(); T=x_ref.shape[1]//CH
    cols=lambda t:slice(T*t,T*(t+1))
    greet_row(p)
    out_sum=Scatter(p,part,s1b,r1b,s2b,r2b,ssem,0)
    y_sum=Scatter(p,part2,s1b,r1b,s2b,r2b,ssem,1)
    da_sum=Scatter(p,part,s1b,r1b,s2b,r2b,ssem,2)
    ga,gy,gd=[Gather(p,b,gsem,i) for i,b in enumerate((a2,dyb,dat))]
    st2,stb=Totals(p,tout,tgot,tsem,0),Totals(p,tout,tgot,tsem,1)
    turn(wot,wo)
    def project(t):
        part[t]=nt(wot[...],o_ref[T*t:T*(t+1),:])
        out_sum.start(t)
    def residual(t):
        x1=x_ref[:,cols(t)]+out_sum.wait(t)+bo[...]
        x1b[t]=x1
        st2.start(t,x1,x1*x1)
    def second_norm(t):
        m,sq=st2.wait(t)
        inv=lax.rsqrt(sq-m*m+EPS)
        st[t,0:1]=m; st[t,1:2]=inv
        ga.start(t,((x1b[t]-m)*inv*g2[...]+s2[...]).astype(bf16))
        gy.start(t,cot_ref[:,cols(t)].astype(bf16))
    def hidden(t):
        ga.wait(t); gy.wait(t)
        def tile(r):
            h=nn(wut[r,:],a2[t])+bu[r,:]
            act,slope=gelu_parts(h)
            gb[t,r]=act.astype(bf16)
            dh=(nn(wd[r,:],dyb[t])*slope).astype(bf16)
            dhb[t,r]=dh
            dbu_ref[r,:]+=jnp.sum(dh.astype(f32),axis=1,keepdims=True)
        tiled(wut.shape[0],128,tile)
        def back(r):
            part[t,r]=nn(wu[r,:],dhb[t])
        tiled(wu.shape[0],256,back)
        da_sum.start(t)
    def down(t):
        def tile(r):
            part2[t,r]=nn(wdt[r,:],gb[t])
        tiled(wdt.shape[0],256,tile)
        y_sum.start(t)
    def norm_of(t): return (x1b[t]-st[t,0:1])*st[t,1:2]
    def second_back(t):
        da2=da_sum.wait(t); norm=norm_of(t)
        dg2_ref[...]+=jnp.sum(da2*norm,axis=1,keepdims=True)
        ds2_ref[...]+=jnp.sum(da2,axis=1,keepdims=True)
        e=da2*g2[...]
        da2b[t]=e
        stb.start(t,e,e*norm)
    def middle(t):
        u,w=stb.wait(t)
        dx1=cot_ref[:,cols(t)]+st[t,1:2]*(da2b[t]-u-norm_of(t)*w)
        dx1_ref[:,cols(t)]=dx1
        low=dx1.astype(bf16)
        dbo_ref[...]+=jnp.sum(low.astype(f32),axis=1,keepdims=True)
        gd.start(t,low)
    def attended(t):
        gd.wait(t)
        do_ref[:,cols(t)]=nn(wo[...],dat[t]).astype(bf16)
    def finish(t):
        y_ref[:,cols(t)]=x1b[t]+y_sum.wait(t)+bd[...]
    for ref in (dg2_ref,ds2_ref,dbo_ref,dbd_ref,dbu_ref): ref[...]=jnp.zeros(ref.shape,f32)
    def weight_grads():
        def one(r):
            acc=None; acc2=None
            for t in range(CH):
                v=nt(gb[t,r],dyb[t]); acc=v if acc is None else acc+v
                v=nt(a2[t,r],dhb[t]); acc2=v if acc2 is None else acc2+v
            dwd_ref[r,:]=acc.astype(bf16)
            dwu_ref[r,:]=acc2.astype(bf16)
        tiled(dwd_ref.shape[0],128,one)
    for t in range(CH): project(t)
    for t in range(CH): out_sum.cross(t)
    turn(wut,wu); turn(wdt,wd)
    for t in range(CH):
        residual(t)
        if t>0: second_norm(t-1)
    second_norm(CH-1)
    for t in range(CH):
        ga.forward(t); gy.forward(t)
        hidden(t)
        if t>0: da_sum.cross(t-1)
    down(0); da_sum.cross(CH-1)
    for t in range(1,CH): down(t)
    for t in range(CH):
        second_back(t)
        if t>0: middle(t-1)
    middle(CH-1)
    for t in range(CH): y_sum.cross(t)
    for t in range(CH): dbd_ref[...]+=jnp.sum(cot_ref[:,cols(t)].astype(bf16).astype(f32),axis=1,keepdims=True)
    for t in range(CH): gd.forward(t)
    weight_grads()
    turned=Turn(p,dwu_ref,tup_ref,usem)
    for t in range(CH): attended(t)
    acc=None
    for t in range(CH):
        v=nt(o_ref[T*t:T*(t+1),:].T,dat[t]); acc=v if acc is None else acc+v
    dwo_ref[...]=acc.astype(bf16)
    for t in range(CH): finish(t)
    turned.wait()
    for c in (out_sum,y_sum,da_sum,ga,gy,gd,st2,stb): c.drain()

def mlp_block(x,cot,o,wo,wu,wd,bo,g2,s2,bu,bd):
    w,n=x.shape; T=n//CH; hid=wu.shape[1]; d=wu.shape[0]
    sd=jax.ShapeDtypeStruct; V=pltpu.VMEM
    return pl.pallas_call(mlp_kernel,name="mlp_block",
      out_shape=(sd((w,n),f32),sd((w,n),f32),sd((w,n),bf16),sd(wo.shape,bf16),sd((hid,d),bf16),sd((4,w,hid),bf16),
                 sd((w,1),f32),sd((w,1),f32),sd((w,1),f32),sd((w,1),f32),sd((hid,1),f32)),
      in_specs=[VM]*11,out_specs=(VM,)*11,
      scratch_shapes=[V((d,w),bf16),V((hid,d),bf16),V((d,hid),bf16),V((CH,d,T),f32),V((CH,d,T),f32),
        V((CH,d,T),bf16),V((CH,d,T),bf16),V((CH,d,T),bf16),V((CH,hid,T),bf16),V((CH,hid,T),bf16),
        V((CH,w,T),f32),V((CH,8,T),f32),V((CH,w,T),f32),
        V((3,CH,2,w,T),bf16),V((3,CH,2,w,T),bf16),V((3,CH,w,T),bf16),V((3,CH,w,T),bf16),
        V((2,CH,8,T),f32),V((2,CH,3,8,T),f32),V((d,hid),bf16),SEM((3,CH,6)),SEM((3,CH,4)),SEM((2,CH,6)),SEM((7,))],
      cost_estimate=pl.CostEstimate(flops=8*10**9,bytes_accessed=3*10**7,transcendentals=10**6),
      compiler_params=pltpu.CompilerParams(collective_id=1,has_side_effects=True,vmem_limit_bytes=60<<20),
    )(x,cot,o,wo,wu,wd,bo,g2,s2,bu,bd)

def local(tokens,cotangent,offsets,ln1_gain,ln1_bias,q_weight,k_weight,v_weight,q_bias,v_bias,rel_pos_h,rel_pos_w,
          out_weight,out_bias,ln2_gain,ln2_bias,up_weight,up_bias,down_weight,down_bias):
    rows=lax.axis_size("row"); r=lax.axis_index("row"); cols=lax.axis_size("col")
    width=tokens.shape[0]; hidden=up_bias.shape[0]//rows
    gather_col=lambda w:lax.all_gather(w.astype(bf16),"col",axis=1,tiled=True)
    per=rows//cols
    def quarters(w):
        n=w.shape[1]//per
        return [w[:,n*i:n*i+n].astype(bf16) for i in range(per)]
    qs=[head_order(a,b,c) for a,b,c in zip(quarters(q_weight),quarters(k_weight),quarters(v_weight))]
    us=quarters(up_weight)
    w_out=gather_col(out_weight); w_down=gather_col(down_weight)
    col=lambda vec,n:own_rows(vec,n,r)[:,None]
    g1,s1,g2,s2=[col(v,width) for v in (ln1_gain,ln1_bias,ln2_gain,ln2_bias)]
    bq=own_rows(q_bias,width,r); bv=own_rows(v_bias,width,r)
    b_qkv=head_order(bq,jnp.zeros_like(bq),bv)[:,None]
    b_out,b_down=col(out_bias,width),col(down_bias,width); b_up=col(up_bias,hidden)
    rel=rel_operands(rel_pos_h,rel_pos_w)
    x=tokens
    a1,qkv,w_qkv,w_up,st1=head_block(x,jnp.stack(qs),jnp.stack(us),g1,s1,b_qkv,cols)
    w_qkv=w_qkv.reshape(D,-1); w_up=w_up.reshape(D,-1)
    o=attend(offsets,qkv,rel)
    output,dx1,do,d_out,d_down,d_up,d_g2,d_s2,d_out_bias,d_down_bias,d_up_bias=mlp_block(
        x,cotangent,o,w_out,w_up,w_down,b_out,g2,s2,b_up,b_down)
    d_g2,d_s2,d_out_bias,d_down_bias,d_up_bias=[v[:,0] for v in (d_g2,d_s2,d_out_bias,d_down_bias,d_up_bias)]
    dqkv,drel=attend_back(offsets,qkv,do,rel)
    b_sums=head_unorder(jnp.sum(dqkv,axis=0,dtype=f32))
    def reduce_col(t,axis): return lax.psum_scatter(t,"col",scatter_dimension=axis,tiled=True)
    early=lax.psum((reduce_col(d_up,0),reduce_col(d_down,1)),"dp")
    input_grad,t_qkv,t_out,d_g1,d_s1=tail_block(dqkv,w_qkv,a1,x,st1,dx1,g1,d_out,cols)
    d_g1,d_s1=d_g1[:,0],d_s1[:,0]
    early,(t_qkv,t_out)=lax.optimization_barrier((early,(t_qkv,t_out)))
    t_qkv,t_out=lax.psum((t_qkv,t_out),"dp")
    t_up,f_down=early[0].astype(f32),early[1].astype(f32)
    f_out=t_out.astype(f32)
    f_up=jnp.concatenate([t_up[i] for i in range(per)],1)
    parts=[head_unorder(t_qkv[i].astype(f32)) for i in range(per)]
    f_q,f_k,f_v=[jnp.concatenate([q[i] for q in parts],1) for i in range(3)]
    dh_rel,dw_rel=rel_grads(drel)
    minor=lax.psum((spread(d_g1,D,r),spread(d_s1,D,r),spread(b_sums[0],D,r),spread(b_sums[2],D,r),dh_rel,dw_rel,
      spread(d_out_bias,D,r),spread(d_g2,D,r),spread(d_s2,D,r),spread(d_up_bias,up_bias.shape[0],r),spread(d_down_bias,D,r)),("dp","row","col"))
    return (output,input_grad,minor[0],minor[1],f_q,f_k,f_v,minor[2],minor[3],minor[4],minor[5],f_out,minor[6],minor[7],
            minor[8],f_up,minor[9],f_down,minor[10])

def solution(mesh):
    act=P("row",("dp","col")); mat=P("row","col"); rep=P()
    return jax.shard_map(local,mesh=mesh,
      in_specs=(act,act,P(("dp","col"),None),rep,rep,mat,mat,mat,rep,rep,rep,rep,mat,rep,rep,rep,mat,rep,mat,rep),
      out_specs=(act,act,rep,rep,mat,mat,mat,rep,rep,rep,rep,mat,rep,rep,rep,mat,rep,mat,rep),check_vma=False)
```
